32 devices in a mesh: dp: 1 (over z), sp: 32 (over y, x, core).
Axes of the slice: x: 4, y: 4, z: 1, core: 2. Of those that a mesh axis runs over, the one named last changes fastest.
The devices are a block of a 4x4x8 slice.
Arguments:
- tokens: bfloat16 [8192, 2048], P(('dp', 'sp'))
- w_q: bfloat16 [2048, 2048], replicated
- w_k: bfloat16 [2048, 2048], replicated
- w_v: bfloat16 [2048, 2048], replicated
- w_o: bfloat16 [2048, 2048], replicated
- grad_y: bfloat16 [8192, 2048], P(('dp', 'sp'))
Outputs:
- output 1: bfloat16 [8192, 2048], P(('dp', 'sp'))
- output 2: bfloat16 [8192, 2048], P(('dp', 'sp'))
- output 3: float32 [2048, 2048], P('dp')
- output 4: float32 [2048, 2048], P('dp')
- output 5: float32 [2048, 2048], P('dp')
- output 6: float32 [2048, 2048], P('dp')
All inputs are finite; a program needn't handle non-finite values.
Results may differ from the reference program's by a relative error of at most 0.00456876.
Values are sent between devices in bfloat16 or wider.
A program may use at most 768 MiB of HBM per device.

```python
import math
import jax
import jax.numpy as jnp

SEQ_LEN = 8192
MODEL_DIM = 2048
HEAD_DIM = 128
BLOCK_LEN = 128


def setup_inputs(seed: int = 0, part: int = 0) -> dict:
    part_key = jax.random.fold_in(jax.random.key(seed), part)
    key_x, key_dy = jax.random.split(part_key)
    key_q, key_k, key_v, key_o = jax.random.split(jax.random.key(seed + 1), 4)
    w_scale = MODEL_DIM ** -0.5
    shape_w = (MODEL_DIM, MODEL_DIM)

    def normal_weight(key_w):
        return (jax.random.normal(key_w, shape_w, jnp.float32) * w_scale).astype(jnp.bfloat16)

    tokens = jax.random.normal(key_x, (SEQ_LEN, MODEL_DIM), jnp.float32)
    grad_y = jax.random.normal(key_dy, (SEQ_LEN, MODEL_DIM), jnp.float32) * SEQ_LEN ** -0.25
    return {"tokens": tokens.astype(jnp.bfloat16), "w_q": normal_weight(key_q), "w_k": normal_weight(key_k), "w_v": normal_weight(key_v), "w_o": normal_weight(key_o), "grad_y": grad_y.astype(jnp.bfloat16)}


def reference(tokens, w_q, w_k, w_v, w_o, grad_y):
    n_heads = MODEL_DIM // HEAD_DIM
    n_blocks = SEQ_LEN // BLOCK_LEN
    att_scale = 1.0 / math.sqrt(SEQ_LEN * HEAD_DIM)
    causal = jnp.arange(BLOCK_LEN)[:, None] >= jnp.arange(BLOCK_LEN)[None, :]

    def project(operand, weight):
        return jnp.dot(operand, weight, preferred_element_type=jnp.float32).astype(jnp.bfloat16)

    def split_heads(tensor):
        return tensor.reshape(n_blocks, BLOCK_LEN, n_heads, HEAD_DIM).astype(jnp.float32)

    def to_rows(tensor):
        return (tensor * att_scale).astype(jnp.bfloat16).reshape(SEQ_LEN, MODEL_DIM)

    def as_bf16(tensor):
        return tensor.astype(jnp.bfloat16).astype(jnp.float32)

    def excl_prefix(blocks):
        zero_block = jnp.zeros_like(blocks[:1])
        return jnp.concatenate([zero_block, jnp.cumsum(blocks, axis=0)[:-1]], axis=0)

    q_heads = split_heads(project(tokens, w_q))
    k_heads = split_heads(project(tokens, w_k))
    v_heads = split_heads(project(tokens, w_v))
    fwd_state = as_bf16(excl_prefix(jnp.einsum("nshd,nshe->nhde", k_heads, v_heads)))
    masked_scores = as_bf16(jnp.where(causal, jnp.einsum("nthd,nshd->nhts", q_heads, k_heads), 0.0))
    out_rows = to_rows(jnp.einsum("nhts,nshe->nthe", masked_scores, v_heads) + jnp.einsum("nthd,nhde->nthe", q_heads, fwd_state))
    out_y = project(out_rows, w_o)

    do_heads = split_heads(project(grad_y, w_o.T))
    block_qdo = jnp.einsum("nthd,nthe->nhde", q_heads, do_heads)
    rev_state = as_bf16(excl_prefix(block_qdo[::-1])[::-1])
    masked_grads = as_bf16(jnp.where(causal, jnp.einsum("nthe,nshe->nhts", do_heads, v_heads), 0.0))
    dq_rows = to_rows(jnp.einsum("nhts,nshd->nthd", masked_grads, k_heads) + jnp.einsum("nthe,nhde->nthd", do_heads, fwd_state))
    dk_rows = to_rows(jnp.einsum("nhts,nthd->nshd", masked_grads, q_heads) + jnp.einsum("nshe,nhde->nshd", v_heads, rev_state))
    dv_rows = to_rows(jnp.einsum("nhts,nthe->nshe", masked_scores, do_heads) + jnp.einsum("nshd,nhde->nshe", k_heads, rev_state))
    grad_x = (jnp.dot(dq_rows, w_q.T, preferred_element_type=jnp.float32) + jnp.dot(dk_rows, w_k.T, preferred_element_type=jnp.float32) + jnp.dot(dv_rows, w_v.T, preferred_element_type=jnp.float32)).astype(jnp.bfloat16)
    grad_wq = jnp.dot(tokens.T, dq_rows, preferred_element_type=jnp.float32)
    grad_wk = jnp.dot(tokens.T, dk_rows, preferred_element_type=jnp.float32)
    grad_wv = jnp.dot(tokens.T, dv_rows, preferred_element_type=jnp.float32)
    grad_wo = jnp.dot(out_rows.T, grad_y, preferred_element_type=jnp.float32)
    return (out_y, grad_x, grad_wq, grad_wk, grad_wv, grad_wo)
```

```python
import functools
import math
import jax
import jax.numpy as jnp
from jax import lax
from jax.experimental import pallas as pl
from jax.experimental.pallas import tpu as pltpu
from jax.sharding import PartitionSpec as P


HEAD_DIM = 128
BLOCK_LEN = 128
N_CORES = 2
N_GRADS = 4


F32 = jnp.float32
BF16 = jnp.bfloat16
VMEM = pltpu.VMEM


def dot(a, b, dims):
    return lax.dot_general(a, b, ((dims[:1], dims[1:]), ((), ())), preferred_element_type=F32)


def project_kernel(x_ref, dy_ref, wq_ref, wk_ref, wv_ref, wo_ref, q_ref, k_ref, v_ref, do_ref, totals_ref):
    x = x_ref[...]
    q_ref[...] = dot(x, wq_ref[...], (1, 0)).astype(BF16)
    k_ref[...] = dot(x, wk_ref[...], (1, 0)).astype(BF16)
    v_ref[...] = dot(x, wv_ref[...], (1, 0)).astype(BF16)
    do_ref[...] = dot(dy_ref[...], wo_ref[...], (1, 1)).astype(BF16)
    rows = totals_ref.shape[2]
    per_head = HEAD_DIM // rows
    for head in range(q_ref.shape[1] // HEAD_DIM):
        cols = slice(head * HEAD_DIM, (head + 1) * HEAD_DIM)
        kv = dot(k_ref[:, cols], v_ref[:, cols], (0, 0))
        qdo = dot(q_ref[:, cols], do_ref[:, cols], (0, 0))
        for part in range(per_head):
            totals_ref[head * per_head + part, 0] = kv[part * rows : (part + 1) * rows]
            totals_ref[head * per_head + part, 1] = qdo[part * rows : (part + 1) * rows]


def prefix_kernel(parts_ref, out_ref):
    n_parts = parts_ref.shape[0]
    before = jnp.zeros_like(parts_ref[0, 0])
    after = jnp.zeros_like(parts_ref[0, 1])
    for step in range(n_parts):
        last = n_parts - 1 - step
        out_ref[step, 0] = before
        out_ref[last, 1] = after
        before = before + parts_ref[step, 0]
        after = after + parts_ref[last, 1]


def attend_kernel(scale, q_ref, k_ref, v_ref, do_ref, x_ref, dy_ref, state_ref, left_ref, right_ref):
    n_blocks = q_ref.shape[0] // BLOCK_LEN
    left_ref[0] = x_ref[...]
    right_ref[3] = dy_ref[...]
    rows = [pl.ds(b * BLOCK_LEN, BLOCK_LEN) for b in range(n_blocks)]
    fwd = [state_ref[:, 0].reshape(HEAD_DIM, HEAD_DIM)]
    for b in range(n_blocks - 1):
        fwd.append(fwd[-1] + dot(k_ref[rows[b]], v_ref[rows[b]], (0, 0)))
    rev = [state_ref[:, 1].reshape(HEAD_DIM, HEAD_DIM)]
    for b in range(n_blocks - 1, 0, -1):
        rev.insert(0, rev[0] + dot(q_ref[rows[b]], do_ref[rows[b]], (0, 0)))
    shape = (BLOCK_LEN, BLOCK_LEN)
    causal = lax.broadcasted_iota(jnp.int32, shape, 0) >= lax.broadcasted_iota(jnp.int32, shape, 1)
    for b in range(n_blocks):
        q, k, v, do = q_ref[rows[b]], k_ref[rows[b]], v_ref[rows[b]], do_ref[rows[b]]
        s = fwd[b].astype(BF16)
        r = rev[b].astype(BF16)
        att = jnp.where(causal, dot(q, k, (1, 1)), 0.0).astype(BF16)
        d_att = jnp.where(causal, dot(do, v, (1, 1)), 0.0).astype(BF16)
        left_ref[1, rows[b]] = ((dot(att, v, (1, 0)) + dot(q, s, (1, 0))) * scale).astype(BF16)
        right_ref[0, rows[b]] = ((dot(d_att, k, (1, 0)) + dot(do, s, (1, 1))) * scale).astype(BF16)
        right_ref[1, rows[b]] = ((dot(d_att, q, (0, 0)) + dot(v, r, (1, 1))) * scale).astype(BF16)
        right_ref[2, rows[b]] = ((dot(att, do, (0, 0)) + dot(k, r, (1, 0))) * scale).astype(BF16)


def place_kernel(side, step, fresh, *refs):
    blocks = refs[:4]
    grads = refs[4 if fresh else 4 + N_GRADS :][:N_GRADS]
    buf, sem_in, sem_out = refs[-3:]
    index = lax.axis_index("sp")
    core = lax.rem(index, N_CORES)
    col = lax.rem(index // N_CORES, side)
    row = index // (N_CORES * side)
    height = blocks[0].shape[0]
    half = grads[0].shape[0] // 2
    granule = buf.shape[1]
    per_block = height // granule
    jobs = []
    for k, src in enumerate(blocks):
        own, part = k < 2, k % 2
        at = col if part == 0 else row
        c = core if own else 1 - core
        which = lax.rem(at - (1 - 2 * c) * step + 2 * side, side)
        start = part * half + c * height
        for g in range(per_block):
            jobs.append((src.at[pl.ds(g * granule, granule)], which, pl.multiple_of(start + g * granule, granule)))
    for n, (src, which, start) in enumerate(jobs):
        pltpu.make_async_copy(src, buf.at[n], sem_in.at[n]).start()
    for n, (src, which, start) in enumerate(jobs):
        pltpu.make_async_copy(src, buf.at[n], sem_in.at[n]).wait()
        for m in range(N_GRADS):

            @pl.when(which == m)
            def _():
                pltpu.make_async_copy(buf.at[n], grads[m].at[pl.ds(start, granule)], sem_out.at[n]).start()

    for n, (src, which, start) in enumerate(jobs):
        pltpu.make_async_copy(buf.at[n], grads[0].at[pl.ds(0, granule)], sem_out.at[n]).wait()


def solution(mesh):
    n_seq = mesh.shape["sp"]
    side = math.isqrt(n_seq // N_CORES)
    row_spec = P(("dp", "sp"), None)
    grad_spec = P("dp", None)

    def device_at(row, col, core):
        return ((row % side) * side + col % side) * N_CORES + core

    def ring_perm(axis, hops):
        pairs = []
        for row in range(side):
            for col in range(side):
                for core in range(N_CORES):
                    shift = hops * (1 - 2 * core)
                    target = device_at(row, col + shift, core) if axis == "x" else device_at(row + shift, col, core)
                    pairs.append((device_at(row, col, core), target))
        return pairs

    core_perm = [(j, j ^ 1) for j in range(n_seq)]

    def local_layer(tokens, w_q, w_k, w_v, w_o, grad_y):
        n_rows, model_dim = tokens.shape
        n_heads = model_dim // HEAD_DIM
        att_scale = 1.0 / math.sqrt(n_rows * n_seq * HEAD_DIM)
        index = lax.axis_index("sp")
        core = lax.rem(index, N_CORES)
        sign = 1 - 2 * core
        place = {"x": lax.rem(index // N_CORES, side), "y": index // (N_CORES * side)}

        def swap_cores(value):
            return lax.ppermute(value, "sp", perm=core_perm)

        def hop(value, axis, hops):
            return lax.ppermute(value, "sp", perm=ring_perm(axis, hops))

        def at_shift(axis, shift):
            return lax.rem(place[axis] + sign * shift + 2 * side, side)

        def project(operand, weight):
            return jnp.dot(operand, weight, preferred_element_type=F32).astype(BF16)

        def back_proj(rows, weight):
            return jnp.einsum("ne,de->nd", rows, weight, preferred_element_type=F32)

        tile = 2 * HEAD_DIM
        slice_rows = n_heads * HEAD_DIM // n_seq
        per_tile = tile // slice_rows
        full = pl.BlockSpec((n_rows, model_dim), lambda i: (0, 0))
        in_cols = pl.BlockSpec((model_dim, tile), lambda i: (0, i))
        in_rows = pl.BlockSpec((tile, model_dim), lambda i: (i, 0))
        out_cols = pl.BlockSpec((n_rows, tile), lambda i: (0, i))
        act = jax.ShapeDtypeStruct((n_rows, model_dim), BF16)
        q, k, v, do, totals = pl.pallas_call(
            project_kernel,
            grid=(model_dim // tile,),
            in_specs=[full, full, in_cols, in_cols, in_cols, in_rows],
            out_specs=[out_cols] * 4 + [pl.BlockSpec((per_tile, 2, slice_rows, HEAD_DIM), lambda i: (i, 0, 0, 0))],
            out_shape=[act] * 4 + [jax.ShapeDtypeStruct((n_seq, 2, slice_rows, HEAD_DIM), F32)],
            cost_estimate=pl.CostEstimate(flops=8 * n_rows * model_dim * model_dim, bytes_accessed=8 * model_dim * model_dim, transcendentals=0),
            compiler_params=pltpu.CompilerParams(vmem_limit_bytes=48 * 2**20),
            name="project",
        )(tokens, grad_y, w_q, w_k, w_v, w_o)

        parts = lax.all_to_all(totals, "sp", 0, 0)
        prefixes = pl.pallas_call(
            prefix_kernel,
            out_shape=jax.ShapeDtypeStruct(parts.shape, parts.dtype),
            in_specs=[pl.BlockSpec(memory_space=VMEM)],
            out_specs=pl.BlockSpec(memory_space=VMEM),
            cost_estimate=pl.CostEstimate(flops=2 * parts.size, bytes_accessed=8 * parts.size, transcendentals=0),
            name="state_prefix",
        )(parts)
        states = lax.all_to_all(prefixes, "sp", 0, 0)

        head_cols = pl.BlockSpec((n_rows, HEAD_DIM), lambda h: (0, h))
        per_head = HEAD_DIM // slice_rows
        lefts, rights = pl.pallas_call(
            functools.partial(attend_kernel, att_scale),
            grid=(n_heads,),
            in_specs=[head_cols] * 6 + [pl.BlockSpec((per_head, 2, slice_rows, HEAD_DIM), lambda h: (h, 0, 0, 0))],
            out_specs=[pl.BlockSpec((2, n_rows, HEAD_DIM), lambda h: (0, 0, h)), pl.BlockSpec((4, n_rows, HEAD_DIM), lambda h: (0, 0, h))],
            out_shape=[jax.ShapeDtypeStruct((2, n_rows, model_dim), BF16), jax.ShapeDtypeStruct((4, n_rows, model_dim), BF16)],
            cost_estimate=pl.CostEstimate(flops=n_heads * 24 * 2 * 128**3, bytes_accessed=2**24, transcendentals=0),
            name="attend",
        )(q, k, v, do, tokens, grad_y, states)

        half = model_dim // 2
        block = half // N_CORES

        def packet(which, part):
            left = lax.dynamic_index_in_dim(lefts, which // (N_GRADS - 1), 0, keepdims=False)[:, part * half : (part + 1) * half]
            right = lax.dynamic_index_in_dim(rights, which, 0, keepdims=False)
            return jnp.concatenate([left, right], axis=1)

        axes = (("x", "y"), ("y", "x"))
        received = []
        for part, (first, second) in enumerate(axes):
            far = hop(packet(at_shift(first, 2), part), first, 1)
            near = hop(packet(at_shift(first, 1), part), first, 1)
            back = hop(packet(at_shift(first, -1), part), first, -1)
            received.append([packet(place[first], part), near, back, hop(far, first, 1)])

        def block_product(left, right):
            return jnp.einsum("nd,ne->de", left, right, preferred_element_type=F32)

        sums = []
        for part in range(2):
            total = None
            for pack in received[part]:
                left, right = pack[:, :half], pack[:, half:]
                mine = lax.dynamic_slice_in_dim(left, core * block, block, 1)
                yours = lax.dynamic_slice_in_dim(left, (1 - core) * block, block, 1)
                other = swap_cores(jnp.concatenate([yours, right], axis=1))
                here = block_product(mine, right)
                total = here if total is None else total + here
                total = total + block_product(other[:, :block], other[:, block:])
            sums.append(total)

        piece = block // side
        pieces = [None, None]
        for step in range(side):
            for part, (first, second) in enumerate(axes):
                own = lax.dynamic_slice_in_dim(sums[part], at_shift(second, -(step + 1)) * piece, piece, 0)
                pieces[part] = own if step == 0 else pieces[part] + own
                if step < side - 1:
                    pieces[part] = hop(pieces[part], second, 1)

        blocks = [jnp.zeros((block, model_dim), F32) for _ in axes]
        for step in range(side):
            for part, (first, second) in enumerate(axes):
                if step:
                    pieces[part] = hop(pieces[part], second, 1)
                blocks[part] = lax.dynamic_update_slice_in_dim(blocks[part], pieces[part], at_shift(second, -step) * piece, 0)

        grads = []
        granule = 128
        n_copies = 4 * block // granule
        for step in range(side):
            if step:
                for part, (first, second) in enumerate(axes):
                    blocks[part] = hop(blocks[part], first, 1)
            others = [swap_cores(b) for b in blocks]
            place_blocks = pl.pallas_call(
                functools.partial(place_kernel, side, step, step == 0),
                in_specs=[pl.BlockSpec(memory_space=pl.ANY)] * (4 + len(grads)),
                out_specs=[pl.BlockSpec(memory_space=pl.ANY)] * N_GRADS,
                out_shape=[jax.ShapeDtypeStruct((model_dim, model_dim), F32)] * N_GRADS,
                scratch_shapes=[VMEM((n_copies, granule, model_dim), F32), pltpu.SemaphoreType.DMA((n_copies,)), pltpu.SemaphoreType.DMA((n_copies,))],
                input_output_aliases={} if step == 0 else {4 + m: m for m in range(N_GRADS)},
                cost_estimate=pl.CostEstimate(flops=5 * 10**9, bytes_accessed=8 * 4 * block * model_dim, transcendentals=0),
            )
            grads = place_blocks(*blocks, *others, *grads)

        out_y = project(lefts[1], w_o)
        grad_x = (back_proj(rights[0], w_q) + back_proj(rights[1], w_k) + back_proj(rights[2], w_v)).astype(BF16)
        return (out_y, grad_x) + tuple(grads)

    return jax.shard_map(local_layer, mesh=mesh, in_specs=(row_spec, P(), P(), P(), P(), row_spec), out_specs=(row_spec, row_spec, grad_spec, grad_spec, grad_spec, grad_spec), check_vma=False)
```

```python
import functools
import math
import jax
import jax.numpy as jnp
from jax import lax
from jax.experimental import pallas as pl
from jax.experimental.pallas import tpu as pltpu
from jax.sharding import PartitionSpec as P


HEAD_DIM = 128
BLOCK_LEN = 128
N_CORES = 2
N_GRADS = 4


F32 = jnp.float32
BF16 = jnp.bfloat16
VMEM = pltpu.VMEM
MESH = pl.DeviceIdType.MESH


def dot(a, b, dims):
    return lax.dot_general(a, b, ((dims[:1], dims[1:]), ((), ())), preferred_element_type=F32)


def project_kernel(x_ref, dy_ref, wq_ref, wk_ref, wv_ref, wo_ref, q_ref, k_ref, v_ref, do_ref, totals_ref):
    x = x_ref[...]
    q_ref[...] = dot(x, wq_ref[...], (1, 0)).astype(BF16)
    k_ref[...] = dot(x, wk_ref[...], (1, 0)).astype(BF16)
    v_ref[...] = dot(x, wv_ref[...], (1, 0)).astype(BF16)
    do_ref[...] = dot(dy_ref[...], wo_ref[...], (1, 1)).astype(BF16)
    rows = totals_ref.shape[2]
    per_head = HEAD_DIM // rows
    for head in range(q_ref.shape[1] // HEAD_DIM):
        cols = slice(head * HEAD_DIM, (head + 1) * HEAD_DIM)
        kv = dot(k_ref[:, cols], v_ref[:, cols], (0, 0))
        qdo = dot(q_ref[:, cols], do_ref[:, cols], (0, 0))
        for part in range(per_head):
            totals_ref[head * per_head + part, 0] = kv[part * rows : (part + 1) * rows]
            totals_ref[head * per_head + part, 1] = qdo[part * rows : (part + 1) * rows]


def prefix_kernel(parts_ref, out_ref):
    n_parts = parts_ref.shape[0]
    before = jnp.zeros_like(parts_ref[0, 0])
    after = jnp.zeros_like(parts_ref[0, 1])
    for step in range(n_parts):
        last = n_parts - 1 - step
        out_ref[step, 0] = before
        out_ref[last, 1] = after
        before = before + parts_ref[step, 0]
        after = after + parts_ref[last, 1]


def attend_kernel(scale, q_ref, k_ref, v_ref, do_ref, x_ref, dy_ref, state_ref, left_ref, right_ref):
    n_blocks = q_ref.shape[0] // BLOCK_LEN
    left_ref[0] = x_ref[...]
    right_ref[3] = dy_ref[...]
    rows = [pl.ds(b * BLOCK_LEN, BLOCK_LEN) for b in range(n_blocks)]
    fwd = [state_ref[:, 0].reshape(HEAD_DIM, HEAD_DIM)]
    for b in range(n_blocks - 1):
        fwd.append(fwd[-1] + dot(k_ref[rows[b]], v_ref[rows[b]], (0, 0)))
    rev = [state_ref[:, 1].reshape(HEAD_DIM, HEAD_DIM)]
    for b in range(n_blocks - 1, 0, -1):
        rev.insert(0, rev[0] + dot(q_ref[rows[b]], do_ref[rows[b]], (0, 0)))
    shape = (BLOCK_LEN, BLOCK_LEN)
    causal = lax.broadcasted_iota(jnp.int32, shape, 0) >= lax.broadcasted_iota(jnp.int32, shape, 1)
    for b in range(n_blocks):
        q, k, v, do = q_ref[rows[b]], k_ref[rows[b]], v_ref[rows[b]], do_ref[rows[b]]
        s = fwd[b].astype(BF16)
        r = rev[b].astype(BF16)
        att = jnp.where(causal, dot(q, k, (1, 1)), 0.0).astype(BF16)
        d_att = jnp.where(causal, dot(do, v, (1, 1)), 0.0).astype(BF16)
        left_ref[1, rows[b]] = ((dot(att, v, (1, 0)) + dot(q, s, (1, 0))) * scale).astype(BF16)
        right_ref[0, rows[b]] = ((dot(d_att, k, (1, 0)) + dot(do, s, (1, 1))) * scale).astype(BF16)
        right_ref[1, rows[b]] = ((dot(d_att, q, (0, 0)) + dot(v, r, (1, 1))) * scale).astype(BF16)
        right_ref[2, rows[b]] = ((dot(att, do, (0, 0)) + dot(k, r, (1, 0))) * scale).astype(BF16)


def exchange_kernel(side, halves, left_ref, right_ref, out0_ref, out1_ref, near_left, near_right, far_left, far_right, pair_left, pair_right, total, landed, gathered, send_sem, recv_sem, ring_send, ring_recv, out_sem):
    me = lax.axis_index("sp")
    core = lax.rem(me, N_CORES)
    sign = 1 - 2 * core
    col = lax.rem(me // N_CORES, side)
    row = me // (N_CORES * side)

    def wrap(value):
        return lax.rem(value + 2 * side, side)

    def device(r, c):
        return (r * side + c) * N_CORES + core

    ahead = (device(row, wrap(col + sign)), device(wrap(row + sign), col))
    behind = (device(row, wrap(col - sign)), device(wrap(row - sign), col))
    partner = me + sign
    at = (col, row)

    barrier = pltpu.get_barrier_semaphore()
    for other in ahead + behind + (partner,):
        pl.semaphore_signal(barrier, inc=1, device_id={"sp": other}, device_id_type=MESH)
    pl.semaphore_wait(barrier, 5)

    half = left_ref.shape[2] // 2
    block = half // N_CORES
    outs = (out0_ref, out1_ref)

    def send(src, dst, send, recv, target):
        copy = pltpu.make_async_remote_copy(src_ref=src, dst_ref=dst, send_sem=send, recv_sem=recv, device_id={"sp": target}, device_id_type=MESH)
        copy.start()
        return copy

    def send_pair(part, kind, left, right, left_dst, right_dst, target):
        return (
            send(right, right_dst, send_sem.at[part, kind, 1], recv_sem.at[part, kind, 1], target),
            send(left, left_dst, send_sem.at[part, kind, 0], recv_sem.at[part, kind, 0], target),
        )

    def left_half(which, part):
        return left_ref.at[which // (N_GRADS - 1), :, pl.ds(part * half, half)]

    def own_left(part, owner):
        start = pl.multiple_of(part * half + owner * block, block)
        return left_ref.at[at[part] // (N_GRADS - 1), :, pl.ds(start, block)]

    copies = {}
    for part in range(2):
        which = wrap(at[part] + 2)
        copies[part, 3] = send_pair(part, 3, left_half(which, part), right_ref.at[which], far_left.at[part], far_right.at[part], ahead[part])
    for part in range(2):
        which = wrap(at[part] - sign)
        copies[part, 1] = send_pair(part, 1, left_half(which, part), right_ref.at[which], near_left.at[part, 1], near_right.at[part, 1], behind[part])
        copies[part, 7] = send_pair(part, 7, own_left(part, 1 - core), right_ref.at[at[part]], pair_left.at[part, 3], pair_right.at[part, 3], partner)
    for part in range(2):
        which = wrap(at[part] + sign)
        copies[part, 0] = send_pair(part, 0, left_half(which, part), right_ref.at[which], near_left.at[part, 0], near_right.at[part, 0], ahead[part])

    def wait_pair(part, kind):
        for copy in copies[part, kind]:
            copy.wait_recv()

    n_tiles = 4
    width = total.shape[2] // n_tiles

    def accumulate(part, left, right, fresh=False):
        left_value = left[...]

        def tile(t, carry):
            cols = pl.ds(pl.multiple_of(t * width, width), width)
            product = dot(left_value, right[:, cols], (0, 0))
            if fresh:
                total[part, :, cols] = product
            else:
                total[part, :, cols] += product
            return carry

        lax.fori_loop(0, n_tiles, tile, 0)

    def my_cols(owner):
        return pl.ds(pl.multiple_of(owner * block, block), block)

    def take(part, slot):
        wait_pair(part, slot)
        packet_left, packet_right = near_left.at[part, slot], near_right.at[part, slot]
        copies[part, 4 + slot] = send_pair(part, 4 + slot, packet_left.at[:, my_cols(1 - core)], packet_right, pair_left.at[part, slot], pair_right.at[part, slot], partner)
        accumulate(part, packet_left.at[:, my_cols(core)], packet_right)

    def take_other(part, slot):
        wait_pair(part, 4 + slot)
        accumulate(part, pair_left.at[part, slot], pair_right.at[part, slot])

    for part in range(2):
        accumulate(part, own_left(part, core), right_ref.at[at[part]], fresh=True)
    for part in range(2):
        take_other(part, 3)
    for part in range(2):
        wait_pair(part, 3)
        copies[part, 2] = send_pair(part, 2, far_left.at[part], far_right.at[part], near_left.at[part, 2], near_right.at[part, 2], ahead[part])
    for slot in (1, 0, 2):
        for part in range(2):
            take(part, slot)
        for part in range(2):
            take_other(part, slot)

    piece = block // side
    small = piece // halves

    def rows(part, shift, h):
        return pl.ds(pl.multiple_of(wrap(at[1 - part] + sign * shift) * piece + h * small, small), small)

    def ring(part, h, step, src, dst):
        return send(src, dst, ring_send.at[part, h, step], ring_recv.at[part, h, step], ahead[1 - part])

    lanes = [(part, h) for h in range(halves) for part in range(2)]
    hops = {}
    for part, h in lanes:
        hops[part, h, 0] = ring(part, h, 0, total.at[part, rows(part, -1, h)], landed.at[part, h, 0])
    for step in range(1, side - 1):
        for part, h in lanes:
            hops[part, h, step - 1].wait_recv()
            landed[part, h, step - 1] += total[part, rows(part, -(step + 1), h), :]
            hops[part, h, step] = ring(part, h, step, landed.at[part, h, step - 1], landed.at[part, h, step])
    stores = []

    def store(part, h, shift, n):
        where = rows(part, shift, h)
        copy = pltpu.make_async_copy(gathered.at[part, where], outs[part].at[where], out_sem.at[part, h, n])
        copy.start()
        stores.append(copy)

    last = side - 1
    for part, h in lanes:
        hops[part, h, last - 1].wait_recv()
        mine = rows(part, 0, h)
        gathered[part, mine, :] = landed[part, h, last - 1] + total[part, mine, :]
        hops[part, h, last] = ring(part, h, last, gathered.at[part, mine], gathered.at[part, mine])
        store(part, h, 0, 0)
    for step in range(1, side):
        for part, h in lanes:
            hops[part, h, last + step - 1].wait_recv()
            where = rows(part, -step, h)
            if step < side - 1:
                hops[part, h, last + step] = ring(part, h, last + step, gathered.at[part, where], gathered.at[part, where])
            store(part, h, -step, step)
    for copy in stores:
        copy.wait()
    for pair in copies.values():
        for copy in pair:
            copy.wait_send()
    for copy in hops.values():
        copy.wait_send()


def place_kernel(side, step, fresh, *refs):
    blocks = refs[:4]
    grads = refs[4 if fresh else 4 + N_GRADS :][:N_GRADS]
    buf, sem_in, sem_out = refs[-3:]
    index = lax.axis_index("sp")
    core = lax.rem(index, N_CORES)
    col = lax.rem(index // N_CORES, side)
    row = index // (N_CORES * side)
    height = blocks[0].shape[0]
    half = grads[0].shape[0] // 2
    granule = buf.shape[1]
    per_block = height // granule
    jobs = []
    for k, src in enumerate(blocks):
        own, part = k < 2, k % 2
        at = col if part == 0 else row
        c = core if own else 1 - core
        which = lax.rem(at - (1 - 2 * c) * step + 2 * side, side)
        start = part * half + c * height
        for g in range(per_block):
            jobs.append((src.at[pl.ds(g * granule, granule)], which, pl.multiple_of(start + g * granule, granule)))
    for n, (src, which, start) in enumerate(jobs):
        pltpu.make_async_copy(src, buf.at[n], sem_in.at[n]).start()
    for n, (src, which, start) in enumerate(jobs):
        pltpu.make_async_copy(src, buf.at[n], sem_in.at[n]).wait()
        for m in range(N_GRADS):

            @pl.when(which == m)
            def _():
                pltpu.make_async_copy(buf.at[n], grads[m].at[pl.ds(start, granule)], sem_out.at[n]).start()

    for n, (src, which, start) in enumerate(jobs):
        pltpu.make_async_copy(buf.at[n], grads[0].at[pl.ds(0, granule)], sem_out.at[n]).wait()


def solution(mesh):
    n_seq = mesh.shape["sp"]
    side = math.isqrt(n_seq // N_CORES)
    row_spec = P(("dp", "sp"), None)
    grad_spec = P("dp", None)

    def device_at(row, col, core):
        return ((row % side) * side + col % side) * N_CORES + core

    def ring_perm(axis, hops):
        pairs = []
        for row in range(side):
            for col in range(side):
                for core in range(N_CORES):
                    shift = hops * (1 - 2 * core)
                    target = device_at(row, col + shift, core) if axis == "x" else device_at(row + shift, col, core)
                    pairs.append((device_at(row, col, core), target))
        return pairs

    core_perm = [(j, j ^ 1) for j in range(n_seq)]

    def local_layer(tokens, w_q, w_k, w_v, w_o, grad_y):
        n_rows, model_dim = tokens.shape
        n_heads = model_dim // HEAD_DIM
        att_scale = 1.0 / math.sqrt(n_rows * n_seq * HEAD_DIM)
        index = lax.axis_index("sp")
        core = lax.rem(index, N_CORES)
        place = {"x": lax.rem(index // N_CORES, side), "y": index // (N_CORES * side)}

        def swap_cores(value):
            return lax.ppermute(value, "sp", perm=core_perm)

        def hop(value, axis, hops):
            return lax.ppermute(value, "sp", perm=ring_perm(axis, hops))

        def project(operand, weight):
            return jnp.dot(operand, weight, preferred_element_type=F32).astype(BF16)

        def back_proj(rows, weight):
            return jnp.einsum("ne,de->nd", rows, weight, preferred_element_type=F32)

        tile = 2 * HEAD_DIM
        slice_rows = n_heads * HEAD_DIM // n_seq
        per_tile = tile // slice_rows
        full = pl.BlockSpec((n_rows, model_dim), lambda i: (0, 0))
        in_cols = pl.BlockSpec((model_dim, tile), lambda i: (0, i))
        in_rows = pl.BlockSpec((tile, model_dim), lambda i: (i, 0))
        out_cols = pl.BlockSpec((n_rows, tile), lambda i: (0, i))
        act = jax.ShapeDtypeStruct((n_rows, model_dim), BF16)
        q, k, v, do, totals = pl.pallas_call(
            project_kernel,
            grid=(model_dim // tile,),
            in_specs=[full, full, in_cols, in_cols, in_cols, in_rows],
            out_specs=[out_cols] * 4 + [pl.BlockSpec((per_tile, 2, slice_rows, HEAD_DIM), lambda i: (i, 0, 0, 0))],
            out_shape=[act] * 4 + [jax.ShapeDtypeStruct((n_seq, 2, slice_rows, HEAD_DIM), F32)],
            cost_estimate=pl.CostEstimate(flops=8 * n_rows * model_dim * model_dim, bytes_accessed=8 * model_dim * model_dim, transcendentals=0),
            compiler_params=pltpu.CompilerParams(vmem_limit_bytes=48 * 2**20),
            name="project",
        )(tokens, grad_y, w_q, w_k, w_v, w_o)

        parts = lax.all_to_all(totals, "sp", 0, 0)
        prefixes = pl.pallas_call(
            prefix_kernel,
            out_shape=jax.ShapeDtypeStruct(parts.shape, parts.dtype),
            in_specs=[pl.BlockSpec(memory_space=VMEM)],
            out_specs=pl.BlockSpec(memory_space=VMEM),
            cost_estimate=pl.CostEstimate(flops=2 * parts.size, bytes_accessed=8 * parts.size, transcendentals=0),
            name="state_prefix",
        )(parts)
        states = lax.all_to_all(prefixes, "sp", 0, 0)

        head_cols = pl.BlockSpec((n_rows, HEAD_DIM), lambda h: (0, h))
        per_head = HEAD_DIM // slice_rows
        lefts, rights = pl.pallas_call(
            functools.partial(attend_kernel, att_scale),
            grid=(n_heads,),
            in_specs=[head_cols] * 6 + [pl.BlockSpec((per_head, 2, slice_rows, HEAD_DIM), lambda h: (h, 0, 0, 0))],
            out_specs=[pl.BlockSpec((2, n_rows, HEAD_DIM), lambda h: (0, 0, h)), pl.BlockSpec((4, n_rows, HEAD_DIM), lambda h: (0, 0, h))],
            out_shape=[jax.ShapeDtypeStruct((2, n_rows, model_dim), BF16), jax.ShapeDtypeStruct((4, n_rows, model_dim), BF16)],
            cost_estimate=pl.CostEstimate(flops=n_heads * 24 * 2 * 128**3, bytes_accessed=2**24, transcendentals=0),
            name="attend",
        )(q, k, v, do, tokens, grad_y, states)

        half = model_dim // 2
        block = half // N_CORES
        halves = 2
        small = block // side // halves
        axes = (("x", "y"), ("y", "x"))
        dma = pltpu.SemaphoreType.DMA
        blocks = pl.pallas_call(
            functools.partial(exchange_kernel, side, halves),
            in_specs=[pl.BlockSpec(memory_space=VMEM)] * 2,
            out_specs=[pl.BlockSpec(memory_space=pl.ANY)] * 2,
            out_shape=[jax.ShapeDtypeStruct((block, model_dim), F32)] * 2,
            scratch_shapes=[
                VMEM((2, 3, n_rows, half), BF16),
                VMEM((2, 3, n_rows, model_dim), BF16),
                VMEM((2, n_rows, half), BF16),
                VMEM((2, n_rows, model_dim), BF16),
                VMEM((2, 4, n_rows, block), BF16),
                VMEM((2, 4, n_rows, model_dim), BF16),
                VMEM((2, block, model_dim), F32),
                VMEM((2, halves, side - 1, small, model_dim), F32),
                VMEM((2, block, model_dim), F32),
                dma((2, 8, 2)),
                dma((2, 8, 2)),
                dma((2, halves, 2 * (side - 1))),
                dma((2, halves, 2 * (side - 1))),
                dma((2, halves, side)),
            ],
            cost_estimate=pl.CostEstimate(flops=2 * 2 * block * model_dim * n_rows * 8, bytes_accessed=2**24, transcendentals=0),
            compiler_params=pltpu.CompilerParams(collective_id=1, has_side_effects=True, vmem_limit_bytes=60 * 2**20),
            name="exchange",
        )(lefts, rights)
        blocks = list(blocks)

        grads = []
        granule = 128
        n_copies = 4 * block // granule
        for step in range(side):
            if step:
                for part, (first, second) in enumerate(axes):
                    blocks[part] = hop(blocks[part], first, 1)
            others = [swap_cores(b) for b in blocks]
            place_blocks = pl.pallas_call(
                functools.partial(place_kernel, side, step, step == 0),
                in_specs=[pl.BlockSpec(memory_space=pl.ANY)] * (4 + len(grads)),
                out_specs=[pl.BlockSpec(memory_space=pl.ANY)] * N_GRADS,
                out_shape=[jax.ShapeDtypeStruct((model_dim, model_dim), F32)] * N_GRADS,
                scratch_shapes=[VMEM((n_copies, granule, model_dim), F32), pltpu.SemaphoreType.DMA((n_copies,)), pltpu.SemaphoreType.DMA((n_copies,))],
                input_output_aliases={} if step == 0 else {4 + m: m for m in range(N_GRADS)},
                cost_estimate=pl.CostEstimate(flops=5 * 10**9, bytes_accessed=8 * 4 * block * model_dim, transcendentals=0),
            )
            grads = place_blocks(*blocks, *others, *grads)

        out_y = project(lefts[1], w_o)
        grad_x = (back_proj(rights[0], w_q) + back_proj(rights[1], w_k) + back_proj(rights[2], w_v)).astype(BF16)
        return (out_y, grad_x) + tuple(grads)

    return jax.shard_map(local_layer, mesh=mesh, in_specs=(row_spec, P(), P(), P(), P(), row_spec), out_specs=(row_spec, row_spec, grad_spec, grad_spec, grad_spec, grad_spec), check_vma=False)
```

```python
import functools
import math
import jax
import jax.numpy as jnp
from jax import lax
from jax.experimental import pallas as pl
from jax.experimental.pallas import tpu as pltpu
from jax.sharding import PartitionSpec as P


HEAD_DIM = 128
BLOCK_LEN = 128
N_CORES = 2
N_GRADS = 4


F32 = jnp.float32
BF16 = jnp.bfloat16
VMEM = pltpu.VMEM
MESH = pl.DeviceIdType.MESH


def dot(a, b, dims):
    return lax.dot_general(a, b, ((dims[:1], dims[1:]), ((), ())), preferred_element_type=F32)


def project_kernel(x_ref, dy_ref, wq_ref, wk_ref, wv_ref, wo_ref, q_ref, k_ref, v_ref, do_ref, totals_ref):
    x = x_ref[...]
    q_ref[...] = dot(x, wq_ref[...], (1, 0)).astype(BF16)
    k_ref[...] = dot(x, wk_ref[...], (1, 0)).astype(BF16)
    v_ref[...] = dot(x, wv_ref[...], (1, 0)).astype(BF16)
    do_ref[...] = dot(dy_ref[...], wo_ref[...], (1, 1)).astype(BF16)
    rows = totals_ref.shape[2]
    per_head = HEAD_DIM // rows
    for head in range(q_ref.shape[1] // HEAD_DIM):
        cols = slice(head * HEAD_DIM, (head + 1) * HEAD_DIM)
        kv = dot(k_ref[:, cols], v_ref[:, cols], (0, 0))
        qdo = dot(q_ref[:, cols], do_ref[:, cols], (0, 0))
        for part in range(per_head):
            totals_ref[head * per_head + part, 0] = kv[part * rows : (part + 1) * rows]
            totals_ref[head * per_head + part, 1] = qdo[part * rows : (part + 1) * rows]


def prefix_kernel(parts_ref, out_ref):
    n_parts = parts_ref.shape[0]
    before = jnp.zeros_like(parts_ref[0, 0])
    after = jnp.zeros_like(parts_ref[0, 1])
    for step in range(n_parts):
        last = n_parts - 1 - step
        out_ref[step, 0] = before
        out_ref[last, 1] = after
        before = before + parts_ref[step, 0]
        after = after + parts_ref[last, 1]


def attend_kernel(scale, q_ref, k_ref, v_ref, do_ref, x_ref, dy_ref, state_ref, left_ref, right_ref):
    n_blocks = q_ref.shape[0] // BLOCK_LEN
    left_ref[0] = x_ref[...]
    right_ref[3] = dy_ref[...]
    rows = [pl.ds(b * BLOCK_LEN, BLOCK_LEN) for b in range(n_blocks)]
    fwd = [state_ref[:, 0].reshape(HEAD_DIM, HEAD_DIM)]
    for b in range(n_blocks - 1):
        fwd.append(fwd[-1] + dot(k_ref[rows[b]], v_ref[rows[b]], (0, 0)))
    rev = [state_ref[:, 1].reshape(HEAD_DIM, HEAD_DIM)]
    for b in range(n_blocks - 1, 0, -1):
        rev.insert(0, rev[0] + dot(q_ref[rows[b]], do_ref[rows[b]], (0, 0)))
    shape = (BLOCK_LEN, BLOCK_LEN)
    causal = lax.broadcasted_iota(jnp.int32, shape, 0) >= lax.broadcasted_iota(jnp.int32, shape, 1)
    for b in range(n_blocks):
        q, k, v, do = q_ref[rows[b]], k_ref[rows[b]], v_ref[rows[b]], do_ref[rows[b]]
        s = fwd[b].astype(BF16)
        r = rev[b].astype(BF16)
        att = jnp.where(causal, dot(q, k, (1, 1)), 0.0).astype(BF16)
        d_att = jnp.where(causal, dot(do, v, (1, 1)), 0.0).astype(BF16)
        left_ref[1, rows[b]] = ((dot(att, v, (1, 0)) + dot(q, s, (1, 0))) * scale).astype(BF16)
        right_ref[0, rows[b]] = ((dot(d_att, k, (1, 0)) + dot(do, s, (1, 1))) * scale).astype(BF16)
        right_ref[1, rows[b]] = ((dot(d_att, q, (0, 0)) + dot(v, r, (1, 1))) * scale).astype(BF16)
        right_ref[2, rows[b]] = ((dot(att, do, (0, 0)) + dot(k, r, (1, 0))) * scale).astype(BF16)


def exchange_kernel(side, halves, left_ref, right_ref, *refs):
    own_outs, other_outs = refs[: 2 * halves], refs[2 * halves : 4 * halves]
    near_left, near_right, far_left, far_right, pair_left, pair_right, total, landed, gathered = refs[4 * halves : -7]
    send_sem, recv_sem, ring_send, ring_recv, out_sem, swap_send, swap_recv = refs[-7:]
    me = lax.axis_index("sp")
    core = lax.rem(me, N_CORES)
    sign = 1 - 2 * core
    col = lax.rem(me // N_CORES, side)
    row = me // (N_CORES * side)

    def wrap(value):
        return lax.rem(value + 2 * side, side)

    def device(r, c):
        return (r * side + c) * N_CORES + core

    ahead = (device(row, wrap(col + sign)), device(wrap(row + sign), col))
    behind = (device(row, wrap(col - sign)), device(wrap(row - sign), col))
    partner = me + sign
    at = (col, row)

    barrier = pltpu.get_barrier_semaphore()
    for other in ahead + behind + (partner,):
        pl.semaphore_signal(barrier, inc=1, device_id={"sp": other}, device_id_type=MESH)
    pl.semaphore_wait(barrier, 5)

    half = left_ref.shape[2] // 2
    block = half // N_CORES

    def send(src, dst, send, recv, target):
        copy = pltpu.make_async_remote_copy(src_ref=src, dst_ref=dst, send_sem=send, recv_sem=recv, device_id={"sp": target}, device_id_type=MESH)
        copy.start()
        return copy

    def send_pair(part, kind, left, right, left_dst, right_dst, target):
        return (
            send(right, right_dst, send_sem.at[part, kind, 1], recv_sem.at[part, kind, 1], target),
            send(left, left_dst, send_sem.at[part, kind, 0], recv_sem.at[part, kind, 0], target),
        )

    def left_half(which, part):
        return left_ref.at[which // (N_GRADS - 1), :, pl.ds(part * half, half)]

    def own_left(part, owner):
        start = pl.multiple_of(part * half + owner * block, block)
        return left_ref.at[at[part] // (N_GRADS - 1), :, pl.ds(start, block)]

    copies = {}
    for part in range(2):
        which = wrap(at[part] + 2)
        copies[part, 3] = send_pair(part, 3, left_half(which, part), right_ref.at[which], far_left.at[part], far_right.at[part], ahead[part])
    for part in range(2):
        which = wrap(at[part] - sign)
        copies[part, 1] = send_pair(part, 1, left_half(which, part), right_ref.at[which], near_left.at[part, 1], near_right.at[part, 1], behind[part])
        copies[part, 7] = send_pair(part, 7, own_left(part, 1 - core), right_ref.at[at[part]], pair_left.at[part, 3], pair_right.at[part, 3], partner)
    for part in range(2):
        which = wrap(at[part] + sign)
        copies[part, 0] = send_pair(part, 0, left_half(which, part), right_ref.at[which], near_left.at[part, 0], near_right.at[part, 0], ahead[part])

    def wait_pair(part, kind):
        for copy in copies[part, kind]:
            copy.wait_recv()

    n_tiles = 4
    width = total.shape[2] // n_tiles

    def accumulate(part, left, right, fresh=False):
        left_value = left[...]

        def tile(t, carry):
            cols = pl.ds(pl.multiple_of(t * width, width), width)
            product = dot(left_value, right[:, cols], (0, 0))
            if fresh:
                total[part, :, cols] = product
            else:
                total[part, :, cols] += product
            return carry

        lax.fori_loop(0, n_tiles, tile, 0)

    def my_cols(owner):
        return pl.ds(pl.multiple_of(owner * block, block), block)

    def take(part, slot):
        wait_pair(part, slot)
        packet_left, packet_right = near_left.at[part, slot], near_right.at[part, slot]
        copies[part, 4 + slot] = send_pair(part, 4 + slot, packet_left.at[:, my_cols(1 - core)], packet_right, pair_left.at[part, slot], pair_right.at[part, slot], partner)
        accumulate(part, packet_left.at[:, my_cols(core)], packet_right)

    def take_other(part, slot):
        wait_pair(part, 4 + slot)
        accumulate(part, pair_left.at[part, slot], pair_right.at[part, slot])

    for part in range(2):
        accumulate(part, own_left(part, core), right_ref.at[at[part]], fresh=True)
    for part in range(2):
        take_other(part, 3)
    for part in range(2):
        wait_pair(part, 3)
        copies[part, 2] = send_pair(part, 2, far_left.at[part], far_right.at[part], near_left.at[part, 2], near_right.at[part, 2], ahead[part])
    for slot in (1, 0, 2):
        for part in range(2):
            take(part, slot)
        for part in range(2):
            take_other(part, slot)

    piece = block // side
    small = piece // halves

    def rows(part, shift, h):
        return pl.ds(pl.multiple_of(wrap(at[1 - part] + sign * shift) * piece + h * small, small), small)

    def ring(part, h, step, src, dst):
        return send(src, dst, ring_send.at[part, h, step], ring_recv.at[part, h, step], ahead[1 - part])

    lanes = [(part, h) for h in range(halves) for part in range(2)]
    hops = {}
    for part, h in lanes:
        hops[part, h, 0] = ring(part, h, 0, total.at[part, rows(part, -1, h)], landed.at[part, h, 0])
    for step in range(1, side - 1):
        for part, h in lanes:
            hops[part, h, step - 1].wait_recv()
            landed[part, h, step - 1] += total[part, rows(part, -(step + 1), h), :]
            hops[part, h, step] = ring(part, h, step, landed.at[part, h, step - 1], landed.at[part, h, step])
    stores = []

    swaps = []

    def store(part, h, shift, n):
        src = gathered.at[part, rows(part, shift, h)]
        where = pl.ds(pl.multiple_of(wrap(at[1 - part] + sign * shift) * small, small), small)
        copy = pltpu.make_async_copy(src, own_outs[2 * h + part].at[where], out_sem.at[part, h, n])
        copy.start()
        stores.append(copy)
        swaps.append(send(src, other_outs[2 * h + part].at[where], swap_send.at[part, h, n], swap_recv.at[part, h, n], partner))

    last = side - 1
    for part, h in lanes:
        hops[part, h, last - 1].wait_recv()
        mine = rows(part, 0, h)
        gathered[part, mine, :] = landed[part, h, last - 1] + total[part, mine, :]
        hops[part, h, last] = ring(part, h, last, gathered.at[part, mine], gathered.at[part, mine])
        store(part, h, 0, 0)
    for step in range(1, side):
        for part, h in lanes:
            hops[part, h, last + step - 1].wait_recv()
            where = rows(part, -step, h)
            if step < side - 1:
                hops[part, h, last + step] = ring(part, h, last + step, gathered.at[part, where], gathered.at[part, where])
            store(part, h, -step, step)
    for copy in stores:
        copy.wait()
    for pair in copies.values():
        for copy in pair:
            copy.wait_send()
    for copy in hops.values():
        copy.wait_send()
    for copy in swaps:
        copy.wait()


def place_kernel(side, step, lane, halves, fresh, *refs):
    blocks = refs[:4]
    grads = refs[4 if fresh else 4 + N_GRADS :][:N_GRADS]
    buf, sem_in, sem_out = refs[-3:]
    index = lax.axis_index("sp")
    core = lax.rem(index, N_CORES)
    col = lax.rem(index // N_CORES, side)
    row = index // (N_CORES * side)
    small = blocks[0].shape[0] // side
    piece = small * halves
    half = grads[0].shape[0] // 2
    jobs = []
    for k, src in enumerate(blocks):
        own, part = k < 2, k % 2
        at = col if part == 0 else row
        c = core if own else 1 - core
        which = lax.rem(at - (1 - 2 * c) * step + 2 * side, side)
        start = part * half + c * side * piece + lane * small
        for g in range(side):
            jobs.append((src.at[pl.ds(g * small, small)], which, pl.multiple_of(start + g * piece, small)))
    for n, (src, which, start) in enumerate(jobs):
        pltpu.make_async_copy(src, buf.at[n], sem_in.at[n]).start()
    for n, (src, which, start) in enumerate(jobs):
        pltpu.make_async_copy(src, buf.at[n], sem_in.at[n]).wait()
        for m in range(N_GRADS):

            @pl.when(which == m)
            def _():
                pltpu.make_async_copy(buf.at[n], grads[m].at[pl.ds(start, small)], sem_out.at[n]).start()

    for n, (src, which, start) in enumerate(jobs):
        pltpu.make_async_copy(buf.at[n], grads[0].at[pl.ds(0, small)], sem_out.at[n]).wait()


def solution(mesh):
    n_seq = mesh.shape["sp"]
    side = math.isqrt(n_seq // N_CORES)
    row_spec = P(("dp", "sp"), None)
    grad_spec = P("dp", None)

    def device_at(row, col, core):
        return ((row % side) * side + col % side) * N_CORES + core

    def ring_perm(axis, hops):
        pairs = []
        for row in range(side):
            for col in range(side):
                for core in range(N_CORES):
                    shift = hops * (1 - 2 * core)
                    target = device_at(row, col + shift, core) if axis == "x" else device_at(row + shift, col, core)
                    pairs.append((device_at(row, col, core), target))
        return pairs

    core_perm = [(j, j ^ 1) for j in range(n_seq)]

    def local_layer(tokens, w_q, w_k, w_v, w_o, grad_y):
        n_rows, model_dim = tokens.shape
        n_heads = model_dim // HEAD_DIM
        att_scale = 1.0 / math.sqrt(n_rows * n_seq * HEAD_DIM)
        index = lax.axis_index("sp")
        core = lax.rem(index, N_CORES)
        place = {"x": lax.rem(index // N_CORES, side), "y": index // (N_CORES * side)}

        def swap_cores(value):
            return lax.ppermute(value, "sp", perm=core_perm)

        def hop(value, axis, hops):
            return lax.ppermute(value, "sp", perm=ring_perm(axis, hops))

        def project(operand, weight):
            return jnp.dot(operand, weight, preferred_element_type=F32).astype(BF16)

        def back_proj(rows, weight):
            return jnp.einsum("ne,de->nd", rows, weight, preferred_element_type=F32)

        tile = 2 * HEAD_DIM
        slice_rows = n_heads * HEAD_DIM // n_seq
        per_tile = tile // slice_rows
        full = pl.BlockSpec((n_rows, model_dim), lambda i: (0, 0))
        in_cols = pl.BlockSpec((model_dim, tile), lambda i: (0, i))
        in_rows = pl.BlockSpec((tile, model_dim), lambda i: (i, 0))
        out_cols = pl.BlockSpec((n_rows, tile), lambda i: (0, i))
        act = jax.ShapeDtypeStruct((n_rows, model_dim), BF16)
        q, k, v, do, totals = pl.pallas_call(
            project_kernel,
            grid=(model_dim // tile,),
            in_specs=[full, full, in_cols, in_cols, in_cols, in_rows],
            out_specs=[out_cols] * 4 + [pl.BlockSpec((per_tile, 2, slice_rows, HEAD_DIM), lambda i: (i, 0, 0, 0))],
            out_shape=[act] * 4 + [jax.ShapeDtypeStruct((n_seq, 2, slice_rows, HEAD_DIM), F32)],
            cost_estimate=pl.CostEstimate(flops=8 * n_rows * model_dim * model_dim, bytes_accessed=8 * model_dim * model_dim, transcendentals=0),
            compiler_params=pltpu.CompilerParams(vmem_limit_bytes=48 * 2**20),
            name="project",
        )(tokens, grad_y, w_q, w_k, w_v, w_o)

        parts = lax.all_to_all(totals, "sp", 0, 0)
        prefixes = pl.pallas_call(
            prefix_kernel,
            out_shape=jax.ShapeDtypeStruct(parts.shape, parts.dtype),
            in_specs=[pl.BlockSpec(memory_space=VMEM)],
            out_specs=pl.BlockSpec(memory_space=VMEM),
            cost_estimate=pl.CostEstimate(flops=2 * parts.size, bytes_accessed=8 * parts.size, transcendentals=0),
            name="state_prefix",
        )(parts)
        states = lax.all_to_all(prefixes, "sp", 0, 0)

        head_cols = pl.BlockSpec((n_rows, HEAD_DIM), lambda h: (0, h))
        per_head = HEAD_DIM // slice_rows
        lefts, rights = pl.pallas_call(
            functools.partial(attend_kernel, att_scale),
            grid=(n_heads,),
            in_specs=[head_cols] * 6 + [pl.BlockSpec((per_head, 2, slice_rows, HEAD_DIM), lambda h: (h, 0, 0, 0))],
            out_specs=[pl.BlockSpec((2, n_rows, HEAD_DIM), lambda h: (0, 0, h)), pl.BlockSpec((4, n_rows, HEAD_DIM), lambda h: (0, 0, h))],
            out_shape=[jax.ShapeDtypeStruct((2, n_rows, model_dim), BF16), jax.ShapeDtypeStruct((4, n_rows, model_dim), BF16)],
            cost_estimate=pl.CostEstimate(flops=n_heads * 24 * 2 * 128**3, bytes_accessed=2**24, transcendentals=0),
            name="attend",
        )(q, k, v, do, tokens, grad_y, states)

        half = model_dim // 2
        block = half // N_CORES
        halves = 2
        small = block // side // halves
        axes = (("x", "y"), ("y", "x"))
        dma = pltpu.SemaphoreType.DMA
        blocks = pl.pallas_call(
            functools.partial(exchange_kernel, side, halves),
            in_specs=[pl.BlockSpec(memory_space=VMEM)] * 2,
            out_specs=[pl.BlockSpec(memory_space=pl.ANY)] * (4 * halves),
            out_shape=[jax.ShapeDtypeStruct((block // halves, model_dim), F32)] * (4 * halves),
            scratch_shapes=[
                VMEM((2, 3, n_rows, half), BF16),
                VMEM((2, 3, n_rows, model_dim), BF16),
                VMEM((2, n_rows, half), BF16),
                VMEM((2, n_rows, model_dim), BF16),
                VMEM((2, 4, n_rows, block), BF16),
                VMEM((2, 4, n_rows, model_dim), BF16),
                VMEM((2, block, model_dim), F32),
                VMEM((2, halves, side - 1, small, model_dim), F32),
                VMEM((2, block, model_dim), F32),
                dma((2, 8, 2)),
                dma((2, 8, 2)),
                dma((2, halves, 2 * (side - 1))),
                dma((2, halves, 2 * (side - 1))),
                dma((2, halves, side)),
                dma((2, halves, side)),
                dma((2, halves, side)),
            ],
            cost_estimate=pl.CostEstimate(flops=2 * 2 * block * model_dim * n_rows * 8, bytes_accessed=2**24, transcendentals=0),
            compiler_params=pltpu.CompilerParams(collective_id=1, has_side_effects=True, vmem_limit_bytes=60 * 2**20),
            name="exchange",
        )(lefts, rights)
        own = [list(blocks[2 * h : 2 * h + 2]) for h in range(halves)]
        others = [list(blocks[2 * (halves + h) : 2 * (halves + h) + 2]) for h in range(halves)]

        grads = []
        n_copies = 4 * side
        for step in range(side):
            for h in range(halves):
                if step:
                    for part, (first, second) in enumerate(axes):
                        own[h][part] = hop(own[h][part], first, 1)
                    others[h] = [swap_cores(b) for b in own[h]]
                fresh = not grads
                place_blocks = pl.pallas_call(
                    functools.partial(place_kernel, side, step, h, halves, fresh),
                    in_specs=[pl.BlockSpec(memory_space=pl.ANY)] * (4 + len(grads)),
                    out_specs=[pl.BlockSpec(memory_space=pl.ANY)] * N_GRADS,
                    out_shape=[jax.ShapeDtypeStruct((model_dim, model_dim), F32)] * N_GRADS,
                    scratch_shapes=[VMEM((n_copies, small, model_dim), F32), dma((n_copies,)), dma((n_copies,))],
                    input_output_aliases={} if fresh else {4 + m: m for m in range(N_GRADS)},
                    cost_estimate=pl.CostEstimate(flops=3 * 10**9, bytes_accessed=32 * n_copies * small * model_dim, transcendentals=0),
                )
                grads = place_blocks(*own[h], *others[h], *grads)

        out_y = project(lefts[1], w_o)
        grad_x = (back_proj(rights[0], w_q) + back_proj(rights[1], w_k) + back_proj(rights[2], w_v)).astype(BF16)
        return (out_y, grad_x) + tuple(grads)

    return jax.shard_map(local_layer, mesh=mesh, in_specs=(row_spec, P(), P(), P(), P(), row_spec), out_specs=(row_spec, row_spec, grad_spec, grad_spec, grad_spec, grad_spec), check_vma=False)
```

```python
import functools
import math
import jax
import jax.numpy as jnp
from jax import lax
from jax.experimental import pallas as pl
from jax.experimental.pallas import tpu as pltpu
from jax.sharding import PartitionSpec as P


HEAD_DIM = 128
BLOCK_LEN = 128
N_CORES = 2
N_GRADS = 4


F32 = jnp.float32
BF16 = jnp.bfloat16
VMEM = pltpu.VMEM
MESH = pl.DeviceIdType.MESH


def dot(a, b, dims):
    return lax.dot_general(a, b, ((dims[:1], dims[1:]), ((), ())), preferred_element_type=F32)


def project_kernel(x_ref, dy_ref, wq_ref, wk_ref, wv_ref, wo_ref, q_ref, k_ref, v_ref, do_ref, totals_ref):
    x = x_ref[...]
    q_ref[...] = dot(x, wq_ref[...], (1, 0)).astype(BF16)
    k_ref[...] = dot(x, wk_ref[...], (1, 0)).astype(BF16)
    v_ref[...] = dot(x, wv_ref[...], (1, 0)).astype(BF16)
    do_ref[...] = dot(dy_ref[...], wo_ref[...], (1, 1)).astype(BF16)
    for head in range(q_ref.shape[1] // HEAD_DIM):
        cols = slice(head * HEAD_DIM, (head + 1) * HEAD_DIM)
        kv = dot(k_ref[:, cols], v_ref[:, cols], (0, 0))
        qdo = dot(q_ref[:, cols], do_ref[:, cols], (0, 0))
        totals_ref[0, head] = kv
        totals_ref[1, head] = qdo


def chain_kernel(side, totals_ref, out_ref, other, before, stage, above, down, peer, swap_send, swap_recv, row_send, row_recv, above_recv, down_send, cast_send, back_send, back_recv):
    me = lax.axis_index("sp")
    core = lax.rem(me, N_CORES)
    col = lax.rem(me // N_CORES, side)
    row = me // (N_CORES * side)
    partner = me + 1 - 2 * core
    n_group = totals_ref.shape[1] // N_CORES
    mine, yours = core * n_group, (1 - core) * n_group

    def wrap(value):
        return lax.rem(value + 2 * side, side)

    def device(r, c):
        return (wrap(r) * side + wrap(c)) * N_CORES + core

    barrier = pltpu.get_barrier_semaphore()
    others = [device(row, col + t) for t in range(1, side)] + [device(row + 1, col), device(row - 1, col), partner]
    for target in others:
        pl.semaphore_signal(barrier, inc=1, device_id={"sp": target}, device_id_type=MESH)
    pl.semaphore_wait(barrier, len(others))

    def copy(src, dst, send, recv, target):
        return pltpu.make_async_remote_copy(src_ref=src, dst_ref=dst, send_sem=send, recv_sem=recv, device_id={"sp": target}, device_id_type=MESH)

    def swap_copy(kind):
        return copy(totals_ref.at[kind, pl.ds(yours, n_group)], other.at[kind], swap_send.at[kind], swap_recv.at[kind], partner)

    def row_copy(kind, h):
        return copy(stage.at[kind, h], before.at[kind, h], row_send.at[kind, h], row_recv.at[kind, h], device(row, col + 1 - 2 * kind))

    def down_copy(kind, h):
        return copy(down.at[kind, h], above.at[kind, h], down_send.at[kind, h], above_recv.at[kind, h], device(row + 1 - 2 * kind, col))

    def cast_copy(kind, h, t):
        return copy(above.at[kind, h], above.at[kind, h], cast_send.at[kind, h, t - 1], above_recv.at[kind, h], device(row, col + t))

    def back_copy(kind, h):
        return copy(peer.at[kind, h], out_ref.at[kind, mine + h], back_send.at[kind, h], back_recv.at[kind, h], partner)

    def position(kind, coordinate):
        return kind * (side - 1) + (1 - 2 * kind) * coordinate

    for kind in range(2):
        swap_copy(kind).start()
    for kind in range(2):

        @pl.when(position(kind, col) == 0)
        def _():
            before[kind] = jnp.zeros_like(before[kind])

        @pl.when((position(kind, col) == side - 1) & (position(kind, row) == 0))
        def _():
            above[kind] = jnp.zeros_like(above[kind])

    for kind in range(2):
        swap_copy(kind).wait()

    def run(slot, carry):
        for kind in range(2):
            along, across = position(kind, col), position(kind, row)
            h = slot - 2 * along

            @pl.when((h >= 0) & (h < n_group))
            def _():
                @pl.when(along > 0)
                def _():
                    row_copy(kind, h).wait_recv()

                stage[kind, h] = before[kind, h] + (totals_ref[kind, mine + h] + other[kind, h])

                @pl.when(along < side - 1)
                def _():
                    row_copy(kind, h).start()

            g = slot - 2 * (side - 1 + across)

            @pl.when((along == side - 1) & (g >= 0) & (g < n_group))
            def _():
                @pl.when(across > 0)
                def _():
                    down_copy(kind, g).wait_recv()

                @pl.when(across < side - 1)
                def _():
                    down[kind, g] = above[kind, g] + stage[kind, g]
                    down_copy(kind, g).start()

                for t in range(1, side):
                    cast_copy(kind, g, t).start()

        return carry

    lax.fori_loop(0, 4 * (side - 1) + n_group, run, 0)

    def finish(h, carry):
        for kind in range(2):

            @pl.when(position(kind, col) < side - 1)
            def _():
                down_copy(kind, h).wait_recv()

            base = above[kind, h] + before[kind, h]
            own_total, other_total = totals_ref[kind, mine + h], other[kind, h]
            out_ref[kind, mine + h] = jnp.where(core == kind, base, base + other_total)
            peer[kind, h] = jnp.where(core == kind, base + own_total, base)
            back_copy(kind, h).start()
        return carry

    lax.fori_loop(0, n_group, finish, 0)

    def drain(h, carry):
        for kind in range(2):
            along, across = position(kind, col), position(kind, row)
            back_copy(kind, h).wait()

            @pl.when(along < side - 1)
            def _():
                row_copy(kind, h).wait_send()

            @pl.when(along == side - 1)
            def _():
                for t in range(1, side):
                    cast_copy(kind, h, t).wait_send()

                @pl.when(across < side - 1)
                def _():
                    down_copy(kind, h).wait_send()

        return carry

    lax.fori_loop(0, n_group, drain, 0)


def attend_kernel(scale, q_ref, k_ref, v_ref, do_ref, x_ref, dy_ref, state_ref, left_ref, right_ref):
    n_blocks = q_ref.shape[0] // BLOCK_LEN
    left_ref[0] = x_ref[...]
    right_ref[3] = dy_ref[...]
    rows = [pl.ds(b * BLOCK_LEN, BLOCK_LEN) for b in range(n_blocks)]
    fwd = [state_ref[0, 0]]
    for b in range(n_blocks - 1):
        fwd.append(fwd[-1] + dot(k_ref[rows[b]], v_ref[rows[b]], (0, 0)))
    rev = [state_ref[1, 0]]
    for b in range(n_blocks - 1, 0, -1):
        rev.insert(0, rev[0] + dot(q_ref[rows[b]], do_ref[rows[b]], (0, 0)))
    shape = (BLOCK_LEN, BLOCK_LEN)
    causal = lax.broadcasted_iota(jnp.int32, shape, 0) >= lax.broadcasted_iota(jnp.int32, shape, 1)
    for b in range(n_blocks):
        q, k, v, do = q_ref[rows[b]], k_ref[rows[b]], v_ref[rows[b]], do_ref[rows[b]]
        s = fwd[b].astype(BF16)
        r = rev[b].astype(BF16)
        att = jnp.where(causal, dot(q, k, (1, 1)), 0.0).astype(BF16)
        d_att = jnp.where(causal, dot(do, v, (1, 1)), 0.0).astype(BF16)
        left_ref[1, rows[b]] = ((dot(att, v, (1, 0)) + dot(q, s, (1, 0))) * scale).astype(BF16)
        right_ref[0, rows[b]] = ((dot(d_att, k, (1, 0)) + dot(do, s, (1, 1))) * scale).astype(BF16)
        right_ref[1, rows[b]] = ((dot(d_att, q, (0, 0)) + dot(v, r, (1, 1))) * scale).astype(BF16)
        right_ref[2, rows[b]] = ((dot(att, do, (0, 0)) + dot(k, r, (1, 0))) * scale).astype(BF16)


def exchange_kernel(side, halves, left_ref, right_ref, *refs):
    own_outs, other_outs = refs[: 2 * halves], refs[2 * halves : 4 * halves]
    near_left, near_right, far_left, far_right, pair_left, pair_right, total, landed, gathered = refs[4 * halves : -7]
    send_sem, recv_sem, ring_send, ring_recv, out_sem, swap_send, swap_recv = refs[-7:]
    me = lax.axis_index("sp")
    core = lax.rem(me, N_CORES)
    sign = 1 - 2 * core
    col = lax.rem(me // N_CORES, side)
    row = me // (N_CORES * side)

    def wrap(value):
        return lax.rem(value + 2 * side, side)

    def device(r, c):
        return (r * side + c) * N_CORES + core

    ahead = (device(row, wrap(col + sign)), device(wrap(row + sign), col))
    behind = (device(row, wrap(col - sign)), device(wrap(row - sign), col))
    partner = me + sign
    at = (col, row)

    barrier = pltpu.get_barrier_semaphore()
    for other in ahead + behind + (partner,):
        pl.semaphore_signal(barrier, inc=1, device_id={"sp": other}, device_id_type=MESH)
    pl.semaphore_wait(barrier, 5)

    half = left_ref.shape[2] // 2
    block = half // N_CORES

    def send(src, dst, send, recv, target):
        copy = pltpu.make_async_remote_copy(src_ref=src, dst_ref=dst, send_sem=send, recv_sem=recv, device_id={"sp": target}, device_id_type=MESH)
        copy.start()
        return copy

    def send_pair(part, kind, left, right, left_dst, right_dst, target):
        return (
            send(right, right_dst, send_sem.at[part, kind, 1], recv_sem.at[part, kind, 1], target),
            send(left, left_dst, send_sem.at[part, kind, 0], recv_sem.at[part, kind, 0], target),
        )

    def left_half(which, part):
        return left_ref.at[which // (N_GRADS - 1), :, pl.ds(part * half, half)]

    def own_left(part, owner):
        start = pl.multiple_of(part * half + owner * block, block)
        return left_ref.at[at[part] // (N_GRADS - 1), :, pl.ds(start, block)]

    copies = {}
    for part in range(2):
        which = wrap(at[part] + 2)
        copies[part, 3] = send_pair(part, 3, left_half(which, part), right_ref.at[which], far_left.at[part], far_right.at[part], ahead[part])
    for part in range(2):
        which = wrap(at[part] - sign)
        copies[part, 1] = send_pair(part, 1, left_half(which, part), right_ref.at[which], near_left.at[part, 1], near_right.at[part, 1], behind[part])
        copies[part, 7] = send_pair(part, 7, own_left(part, 1 - core), right_ref.at[at[part]], pair_left.at[part, 3], pair_right.at[part, 3], partner)
    for part in range(2):
        which = wrap(at[part] + sign)
        copies[part, 0] = send_pair(part, 0, left_half(which, part), right_ref.at[which], near_left.at[part, 0], near_right.at[part, 0], ahead[part])

    def wait_pair(part, kind):
        for copy in copies[part, kind]:
            copy.wait_recv()

    n_tiles = 4
    width = total.shape[2] // n_tiles

    def accumulate(part, left, right, fresh=False):
        left_value = left[...]

        def tile(t, carry):
            cols = pl.ds(pl.multiple_of(t * width, width), width)
            product = dot(left_value, right[:, cols], (0, 0))
            if fresh:
                total[part, :, cols] = product
            else:
                total[part, :, cols] += product
            return carry

        lax.fori_loop(0, n_tiles, tile, 0)

    def my_cols(owner):
        return pl.ds(pl.multiple_of(owner * block, block), block)

    def take(part, slot):
        wait_pair(part, slot)
        packet_left, packet_right = near_left.at[part, slot], near_right.at[part, slot]
        copies[part, 4 + slot] = send_pair(part, 4 + slot, packet_left.at[:, my_cols(1 - core)], packet_right, pair_left.at[part, slot], pair_right.at[part, slot], partner)
        accumulate(part, packet_left.at[:, my_cols(core)], packet_right)

    def take_other(part, slot):
        wait_pair(part, 4 + slot)
        accumulate(part, pair_left.at[part, slot], pair_right.at[part, slot])

    for part in range(2):
        accumulate(part, own_left(part, core), right_ref.at[at[part]], fresh=True)
    for part in range(2):
        take_other(part, 3)
    for part in range(2):
        wait_pair(part, 3)
        copies[part, 2] = send_pair(part, 2, far_left.at[part], far_right.at[part], near_left.at[part, 2], near_right.at[part, 2], ahead[part])
    for slot in (1, 0, 2):
        for part in range(2):
            take(part, slot)
        for part in range(2):
            take_other(part, slot)

    piece = block // side
    small = piece // halves

    def rows(part, shift, h):
        return pl.ds(pl.multiple_of(wrap(at[1 - part] + sign * shift) * piece + h * small, small), small)

    def ring(part, h, step, src, dst):
        return send(src, dst, ring_send.at[part, h, step], ring_recv.at[part, h, step], ahead[1 - part])

    lanes = [(part, h) for h in range(halves) for part in range(2)]
    hops = {}
    for part, h in lanes:
        hops[part, h, 0] = ring(part, h, 0, total.at[part, rows(part, -1, h)], landed.at[part, h, 0])
    for step in range(1, side - 1):
        for part, h in lanes:
            hops[part, h, step - 1].wait_recv()
            landed[part, h, step - 1] += total[part, rows(part, -(step + 1), h), :]
            hops[part, h, step] = ring(part, h, step, landed.at[part, h, step - 1], landed.at[part, h, step])
    stores = []

    swaps = []

    def store(part, h, shift, n):
        src = gathered.at[part, rows(part, shift, h)]
        where = pl.ds(pl.multiple_of(wrap(at[1 - part] + sign * shift) * small, small), small)
        copy = pltpu.make_async_copy(src, own_outs[2 * h + part].at[where], out_sem.at[part, h, n])
        copy.start()
        stores.append(copy)
        swaps.append(send(src, other_outs[2 * h + part].at[where], swap_send.at[part, h, n], swap_recv.at[part, h, n], partner))

    last = side - 1
    for part, h in lanes:
        hops[part, h, last - 1].wait_recv()
        mine = rows(part, 0, h)
        gathered[part, mine, :] = landed[part, h, last - 1] + total[part, mine, :]
        hops[part, h, last] = ring(part, h, last, gathered.at[part, mine], gathered.at[part, mine])
        store(part, h, 0, 0)
    for step in range(1, side):
        for part, h in lanes:
            hops[part, h, last + step - 1].wait_recv()
            where = rows(part, -step, h)
            if step < side - 1:
                hops[part, h, last + step] = ring(part, h, last + step, gathered.at[part, where], gathered.at[part, where])
            store(part, h, -step, step)
    for copy in stores:
        copy.wait()
    for pair in copies.values():
        for copy in pair:
            copy.wait_send()
    for copy in hops.values():
        copy.wait_send()
    for copy in swaps:
        copy.wait()


def place_kernel(side, step, lane, halves, fresh, *refs):
    blocks = refs[:4]
    grads = refs[4 if fresh else 4 + N_GRADS :][:N_GRADS]
    buf, sem_in, sem_out = refs[-3:]
    index = lax.axis_index("sp")
    core = lax.rem(index, N_CORES)
    col = lax.rem(index // N_CORES, side)
    row = index // (N_CORES * side)
    small = blocks[0].shape[0] // side
    piece = small * halves
    half = grads[0].shape[0] // 2
    jobs = []
    for k, src in enumerate(blocks):
        own, part = k < 2, k % 2
        at = col if part == 0 else row
        c = core if own else 1 - core
        which = lax.rem(at - (1 - 2 * c) * step + 2 * side, side)
        start = part * half + c * side * piece + lane * small
        for g in range(side):
            jobs.append((src.at[pl.ds(g * small, small)], which, pl.multiple_of(start + g * piece, small)))
    for n, (src, which, start) in enumerate(jobs):
        pltpu.make_async_copy(src, buf.at[n], sem_in.at[n]).start()
    for n, (src, which, start) in enumerate(jobs):
        pltpu.make_async_copy(src, buf.at[n], sem_in.at[n]).wait()
        for m in range(N_GRADS):

            @pl.when(which == m)
            def _():
                pltpu.make_async_copy(buf.at[n], grads[m].at[pl.ds(start, small)], sem_out.at[n]).start()

    for n, (src, which, start) in enumerate(jobs):
        pltpu.make_async_copy(buf.at[n], grads[0].at[pl.ds(0, small)], sem_out.at[n]).wait()


def solution(mesh):
    n_seq = mesh.shape["sp"]
    side = math.isqrt(n_seq // N_CORES)
    row_spec = P(("dp", "sp"), None)
    grad_spec = P("dp", None)

    def device_at(row, col, core):
        return ((row % side) * side + col % side) * N_CORES + core

    def ring_perm(axis, hops):
        pairs = []
        for row in range(side):
            for col in range(side):
                for core in range(N_CORES):
                    shift = hops * (1 - 2 * core)
                    target = device_at(row, col + shift, core) if axis == "x" else device_at(row + shift, col, core)
                    pairs.append((device_at(row, col, core), target))
        return pairs

    core_perm = [(j, j ^ 1) for j in range(n_seq)]

    def local_layer(tokens, w_q, w_k, w_v, w_o, grad_y):
        n_rows, model_dim = tokens.shape
        n_heads = model_dim // HEAD_DIM
        att_scale = 1.0 / math.sqrt(n_rows * n_seq * HEAD_DIM)
        index = lax.axis_index("sp")
        core = lax.rem(index, N_CORES)
        place = {"x": lax.rem(index // N_CORES, side), "y": index // (N_CORES * side)}

        def swap_cores(value):
            return lax.ppermute(value, "sp", perm=core_perm)

        def hop(value, axis, hops):
            return lax.ppermute(value, "sp", perm=ring_perm(axis, hops))

        def project(operand, weight):
            return jnp.dot(operand, weight, preferred_element_type=F32).astype(BF16)

        def back_proj(rows, weight):
            return jnp.einsum("ne,de->nd", rows, weight, preferred_element_type=F32)

        tile = 2 * HEAD_DIM
        state_shape = (2, n_heads, HEAD_DIM, HEAD_DIM)
        full = pl.BlockSpec((n_rows, model_dim), lambda i: (0, 0))
        in_cols = pl.BlockSpec((model_dim, tile), lambda i: (0, i))
        in_rows = pl.BlockSpec((tile, model_dim), lambda i: (i, 0))
        out_cols = pl.BlockSpec((n_rows, tile), lambda i: (0, i))
        act = jax.ShapeDtypeStruct((n_rows, model_dim), BF16)
        q, k, v, do, totals = pl.pallas_call(
            project_kernel,
            grid=(model_dim // tile,),
            in_specs=[full, full, in_cols, in_cols, in_cols, in_rows],
            out_specs=[out_cols] * 4 + [pl.BlockSpec((2, tile // HEAD_DIM, HEAD_DIM, HEAD_DIM), lambda i: (0, i, 0, 0))],
            out_shape=[act] * 4 + [jax.ShapeDtypeStruct(state_shape, F32)],
            cost_estimate=pl.CostEstimate(flops=8 * n_rows * model_dim * model_dim, bytes_accessed=8 * model_dim * model_dim, transcendentals=0),
            compiler_params=pltpu.CompilerParams(vmem_limit_bytes=48 * 2**20),
            name="project",
        )(tokens, grad_y, w_q, w_k, w_v, w_o)

        dma = pltpu.SemaphoreType.DMA
        n_group = n_heads // N_CORES
        states = pl.pallas_call(
            functools.partial(chain_kernel, side),
            in_specs=[pl.BlockSpec(memory_space=VMEM)],
            out_specs=pl.BlockSpec(memory_space=VMEM),
            out_shape=jax.ShapeDtypeStruct(state_shape, F32),
            scratch_shapes=[VMEM((2, n_group, HEAD_DIM, HEAD_DIM), F32)] * 6
            + [dma((2,))] * 2
            + [dma((2, n_group))] * 4
            + [dma((2, n_group, side - 1))]
            + [dma((2, n_group))] * 2,
            cost_estimate=pl.CostEstimate(flops=10**8, bytes_accessed=2**22, transcendentals=0),
            compiler_params=pltpu.CompilerParams(collective_id=2, has_side_effects=True),
            name="state_chain",
        )(totals)

        head_cols = pl.BlockSpec((n_rows, HEAD_DIM), lambda h: (0, h))
        lefts, rights = pl.pallas_call(
            functools.partial(attend_kernel, att_scale),
            grid=(n_heads,),
            in_specs=[head_cols] * 6 + [pl.BlockSpec((2, 1, HEAD_DIM, HEAD_DIM), lambda h: (0, h, 0, 0))],
            out_specs=[pl.BlockSpec((2, n_rows, HEAD_DIM), lambda h: (0, 0, h)), pl.BlockSpec((4, n_rows, HEAD_DIM), lambda h: (0, 0, h))],
            out_shape=[jax.ShapeDtypeStruct((2, n_rows, model_dim), BF16), jax.ShapeDtypeStruct((4, n_rows, model_dim), BF16)],
            cost_estimate=pl.CostEstimate(flops=n_heads * 24 * 2 * 128**3, bytes_accessed=2**24, transcendentals=0),
            name="attend",
        )(q, k, v, do, tokens, grad_y, states)

        half = model_dim // 2
        block = half // N_CORES
        halves = 2
        small = block // side // halves
        axes = (("x", "y"), ("y", "x"))
        blocks = pl.pallas_call(
            functools.partial(exchange_kernel, side, halves),
            in_specs=[pl.BlockSpec(memory_space=VMEM)] * 2,
            out_specs=[pl.BlockSpec(memory_space=pl.ANY)] * (4 * halves),
            out_shape=[jax.ShapeDtypeStruct((block // halves, model_dim), F32)] * (4 * halves),
            scratch_shapes=[
                VMEM((2, 3, n_rows, half), BF16),
                VMEM((2, 3, n_rows, model_dim), BF16),
                VMEM((2, n_rows, half), BF16),
                VMEM((2, n_rows, model_dim), BF16),
                VMEM((2, 4, n_rows, block), BF16),
                VMEM((2, 4, n_rows, model_dim), BF16),
                VMEM((2, block, model_dim), F32),
                VMEM((2, halves, side - 1, small, model_dim), F32),
                VMEM((2, block, model_dim), F32),
                dma((2, 8, 2)),
                dma((2, 8, 2)),
                dma((2, halves, 2 * (side - 1))),
                dma((2, halves, 2 * (side - 1))),
                dma((2, halves, side)),
                dma((2, halves, side)),
                dma((2, halves, side)),
            ],
            cost_estimate=pl.CostEstimate(flops=2 * 2 * block * model_dim * n_rows * 8, bytes_accessed=2**24, transcendentals=0),
            compiler_params=pltpu.CompilerParams(collective_id=1, has_side_effects=True, vmem_limit_bytes=60 * 2**20),
            name="exchange",
        )(lefts, rights)
        own = [list(blocks[2 * h : 2 * h + 2]) for h in range(halves)]
        others = [list(blocks[2 * (halves + h) : 2 * (halves + h) + 2]) for h in range(halves)]

        grads = []
        n_copies = 4 * side
        for step in range(side):
            for h in range(halves):
                if step:
                    for part, (first, second) in enumerate(axes):
                        own[h][part] = hop(own[h][part], first, 1)
                    others[h] = [swap_cores(b) for b in own[h]]
                fresh = not grads
                place_blocks = pl.pallas_call(
                    functools.partial(place_kernel, side, step, h, halves, fresh),
                    in_specs=[pl.BlockSpec(memory_space=pl.ANY)] * (4 + len(grads)),
                    out_specs=[pl.BlockSpec(memory_space=pl.ANY)] * N_GRADS,
                    out_shape=[jax.ShapeDtypeStruct((model_dim, model_dim), F32)] * N_GRADS,
                    scratch_shapes=[VMEM((n_copies, small, model_dim), F32), dma((n_copies,)), dma((n_copies,))],
                    input_output_aliases={} if fresh else {4 + m: m for m in range(N_GRADS)},
                    cost_estimate=pl.CostEstimate(flops=3 * 10**9, bytes_accessed=32 * n_copies * small * model_dim, transcendentals=0),
                )
                grads = place_blocks(*own[h], *others[h], *grads)

        out_y = project(lefts[1], w_o)
        grad_x = back_proj(rights[0], w_q)
        grad_x = grad_x + back_proj(rights[1], w_k)
        grad_x = (grad_x + back_proj(rights[2], w_v)).astype(BF16)
        return (out_y, grad_x) + tuple(grads)

    return jax.shard_map(local_layer, mesh=mesh, in_specs=(row_spec, P(), P(), P(), P(), row_spec), out_specs=(row_spec, row_spec, grad_spec, grad_spec, grad_spec, grad_spec), check_vma=False)
```

```python
import functools
import math
import jax
import jax.numpy as jnp
from jax import lax
from jax.experimental import pallas as pl
from jax.experimental.pallas import tpu as pltpu
from jax.sharding import PartitionSpec as P


HEAD_DIM = 128
BLOCK_LEN = 128
N_CORES = 2
N_GRADS = 4
RELAY_STEP = 7
SLOTS = 2


F32 = jnp.float32
BF16 = jnp.bfloat16
VMEM = pltpu.VMEM
MESH = pl.DeviceIdType.MESH


def dot(a, b, dims):
    return lax.dot_general(a, b, ((dims[:1], dims[1:]), ((), ())), preferred_element_type=F32)


def neighbours(me, side):
    core = lax.rem(me, N_CORES)
    sign = 1 - 2 * core
    col = lax.rem(me // N_CORES, side)
    row = me // (N_CORES * side)

    def wrap(value):
        return lax.rem(value + 2 * side, side)

    def device(r, c):
        return (r * side + c) * N_CORES + core

    ahead = (device(row, wrap(col + sign)), device(wrap(row + sign), col))
    behind = (device(row, wrap(col - sign)), device(wrap(row - sign), col))
    return core, sign, (col, row), ahead, behind, wrap


def remote(src, dst, send, recv, target):
    return pltpu.make_async_remote_copy(src_ref=src, dst_ref=dst, send_sem=send, recv_sem=recv, device_id={"sp": target}, device_id_type=MESH)


def chain(side, totals_ref, out_ref, other, before, stage, above, down, peer, swap_send, swap_recv, row_send, row_recv, above_recv, down_send, cast_send, back_send, back_recv):
    me = lax.axis_index("sp")
    core = lax.rem(me, N_CORES)
    col = lax.rem(me // N_CORES, side)
    row = me // (N_CORES * side)
    partner = me + 1 - 2 * core
    n_group = totals_ref.shape[1] // N_CORES
    mine, yours = core * n_group, (1 - core) * n_group

    def wrap(value):
        return lax.rem(value + 2 * side, side)

    def device(r, c):
        return (wrap(r) * side + wrap(c)) * N_CORES + core

    def copy(src, dst, send, recv, target):
        return pltpu.make_async_remote_copy(src_ref=src, dst_ref=dst, send_sem=send, recv_sem=recv, device_id={"sp": target}, device_id_type=MESH)

    def swap_copy(kind):
        return copy(totals_ref.at[kind, pl.ds(yours, n_group)], other.at[kind], swap_send.at[kind], swap_recv.at[kind], partner)

    def row_copy(kind, h):
        return copy(stage.at[kind, h], before.at[kind, h], row_send.at[kind, h], row_recv.at[kind, h], device(row, col + 1 - 2 * kind))

    def down_copy(kind, h):
        return copy(down.at[kind, h], above.at[kind, h], down_send.at[kind, h], above_recv.at[kind, h], device(row + 1 - 2 * kind, col))

    def cast_copy(kind, h, t):
        return copy(above.at[kind, h], above.at[kind, h], cast_send.at[kind, h, t - 1], above_recv.at[kind, h], device(row, col + t))

    def back_copy(kind, h):
        return copy(peer.at[kind, h], out_ref.at[kind, mine + h], back_send.at[kind, h], back_recv.at[kind, h], partner)

    def position(kind, coordinate):
        return kind * (side - 1) + (1 - 2 * kind) * coordinate

    for kind in range(2):
        swap_copy(kind).start()
    for kind in range(2):

        @pl.when(position(kind, col) == 0)
        def _():
            before[kind] = jnp.zeros_like(before[kind])

        @pl.when((position(kind, col) == side - 1) & (position(kind, row) == 0))
        def _():
            above[kind] = jnp.zeros_like(above[kind])

    for kind in range(2):
        swap_copy(kind).wait()

    def run(slot, carry):
        for kind in range(2):
            along, across = position(kind, col), position(kind, row)
            h = slot - SLOTS * along

            @pl.when((h >= 0) & (h < n_group))
            def _():
                @pl.when(along > 0)
                def _():
                    row_copy(kind, h).wait_recv()

                stage[kind, h] = before[kind, h] + (totals_ref[kind, mine + h] + other[kind, h])

                @pl.when(along < side - 1)
                def _():
                    row_copy(kind, h).start()

            g = slot - SLOTS * (side - 1 + across)

            @pl.when((along == side - 1) & (g >= 0) & (g < n_group))
            def _():
                @pl.when(across > 0)
                def _():
                    down_copy(kind, g).wait_recv()

                @pl.when(across < side - 1)
                def _():
                    down[kind, g] = above[kind, g] + stage[kind, g]
                    down_copy(kind, g).start()

                for t in range(1, side):
                    cast_copy(kind, g, t).start()

        return carry

    lax.fori_loop(0, 2 * SLOTS * (side - 1) + n_group, run, 0)

    def finish(h, carry):
        for kind in range(2):

            @pl.when(position(kind, col) < side - 1)
            def _():
                down_copy(kind, h).wait_recv()

            base = above[kind, h] + before[kind, h]
            own_total, other_total = totals_ref[kind, mine + h], other[kind, h]
            out_ref[kind, mine + h] = jnp.where(core == kind, base, base + other_total)
            peer[kind, h] = jnp.where(core == kind, base + own_total, base)
            back_copy(kind, h).start()
        return carry

    lax.fori_loop(0, n_group, finish, 0)

    def drain(h, carry):
        for kind in range(2):
            along, across = position(kind, col), position(kind, row)
            back_copy(kind, h).wait()

            @pl.when(along < side - 1)
            def _():
                row_copy(kind, h).wait_send()

            @pl.when(along == side - 1)
            def _():
                for t in range(1, side):
                    cast_copy(kind, h, t).wait_send()

                @pl.when(across < side - 1)
                def _():
                    down_copy(kind, h).wait_send()

        return carry

    lax.fori_loop(0, n_group, drain, 0)


def project_kernel(side, x_ref, dy_ref, wq_ref, wk_ref, wv_ref, wo_ref, x_any, dy_any, q_ref, k_ref, v_ref, do_ref, early_ref, states_ref, totals, states, relay, send_sem, recv_sem, own_sem, *chain_refs):
    core, sign, at, ahead, behind, wrap = neighbours(lax.axis_index("sp"), side)
    half = early_ref.shape[3]
    step = pl.program_id(0)

    def early(part, kind, src):
        dst = relay.at[part] if kind == 3 else early_ref.at[part, kind]
        return remote(src, dst, send_sem.at[part, kind], recv_sem.at[part, kind], behind[part] if kind == 1 else ahead[part])

    def source(part, array):
        return array.at[:, pl.ds(part * half, half)]

    def start_to(part, kind, which):
        @pl.when(which < N_GRADS - 1)
        def _():
            early(part, kind, source(part, x_any)).start()

        @pl.when(which == N_GRADS - 1)
        def _():
            early(part, kind, source(part, dy_any)).start()

    def own(part, array):
        return pltpu.make_async_copy(source(part, array), early_ref.at[part, 3], own_sem.at[part])

    @pl.when(step == 0)
    def _():
        barrier = pltpu.get_barrier_semaphore()
        me = lax.axis_index("sp")
        first_in_row = at[1] * side * N_CORES + core
        peers = [first_in_row + wrap(at[0] + t) * N_CORES for t in range(1, side)] + [ahead[1], behind[1], me + sign]
        for target in peers:
            pl.semaphore_signal(barrier, inc=1, device_id={"sp": target}, device_id_type=MESH)
        pl.semaphore_wait(barrier, len(peers))
        for part in range(2):
            start_to(part, 3, wrap(at[part] + 2))
        for part in range(2):
            start_to(part, 1, wrap(at[part] - sign))
        for part in range(2):
            start_to(part, 0, wrap(at[part] + sign))

            @pl.when(at[part] < N_GRADS - 1)
            def _():
                own(part, x_any).start()

            @pl.when(at[part] == N_GRADS - 1)
            def _():
                own(part, dy_any).start()

    @pl.when(step == RELAY_STEP)
    def _():
        for part in range(2):
            early(part, 3, source(part, x_any)).wait_recv()
            early(part, 2, relay.at[part]).start()

    x = x_ref[...]
    q_ref[...] = dot(x, wq_ref[...], (1, 0)).astype(BF16)
    k_ref[...] = dot(x, wk_ref[...], (1, 0)).astype(BF16)
    v_ref[...] = dot(x, wv_ref[...], (1, 0)).astype(BF16)
    do_ref[...] = dot(dy_ref[...], wo_ref[...], (1, 1)).astype(BF16)
    for head in range(q_ref.shape[1] // HEAD_DIM):
        cols = slice(head * HEAD_DIM, (head + 1) * HEAD_DIM)
        kv = dot(k_ref[:, cols], v_ref[:, cols], (0, 0))
        qdo = dot(q_ref[:, cols], do_ref[:, cols], (0, 0))
        at_head = step * (q_ref.shape[1] // HEAD_DIM) + head
        totals[0, at_head] = kv
        totals[1, at_head] = qdo

    @pl.when(step == pl.num_programs(0) - 1)
    def _():
        chain(side, totals, states, *chain_refs)
        result = pltpu.make_async_copy(states, states_ref, own_sem.at[2])
        result.start()
        result.wait()
        for part in range(2):
            own(part, x_any).wait()
            for kind in range(4):
                copy = early(part, kind, source(part, x_any))
                copy.wait_send()
                if kind != 3:
                    copy.wait_recv()


def attend_kernel(scale, q_ref, k_ref, v_ref, do_ref, dy_ref, state_ref, out_ref, late_ref):
    n_blocks = q_ref.shape[0] // BLOCK_LEN
    rows = [pl.ds(b * BLOCK_LEN, BLOCK_LEN) for b in range(n_blocks)]
    fwd = [state_ref[0, 0]]
    for b in range(n_blocks - 1):
        fwd.append(fwd[-1] + dot(k_ref[rows[b]], v_ref[rows[b]], (0, 0)))
    rev = [state_ref[1, 0]]
    for b in range(n_blocks - 1, 0, -1):
        rev.insert(0, rev[0] + dot(q_ref[rows[b]], do_ref[rows[b]], (0, 0)))
    shape = (BLOCK_LEN, BLOCK_LEN)
    causal = lax.broadcasted_iota(jnp.int32, shape, 0) >= lax.broadcasted_iota(jnp.int32, shape, 1)
    for b in range(n_blocks):
        q, k, v, do = q_ref[rows[b]], k_ref[rows[b]], v_ref[rows[b]], do_ref[rows[b]]
        s = fwd[b].astype(BF16)
        r = rev[b].astype(BF16)
        att = jnp.where(causal, dot(q, k, (1, 1)), 0.0).astype(BF16)
        d_att = jnp.where(causal, dot(do, v, (1, 1)), 0.0).astype(BF16)
        out_ref[rows[b], :] = ((dot(att, v, (1, 0)) + dot(q, s, (1, 0))) * scale).astype(BF16)
        late_ref[0, rows[b]] = ((dot(d_att, k, (1, 0)) + dot(do, s, (1, 1))) * scale).astype(BF16)
        late_ref[1, rows[b]] = ((dot(d_att, q, (0, 0)) + dot(v, r, (1, 1))) * scale).astype(BF16)
        late_ref[2, rows[b]] = ((dot(att, do, (0, 0)) + dot(k, r, (1, 0))) * scale).astype(BF16)
    first_half = pl.program_id(0) < pl.num_programs(0) // 2

    @pl.when(first_half)
    def _():
        late_ref[3] = out_ref[...]
        late_ref[4] = dy_ref[...]

    @pl.when(jnp.logical_not(first_half))
    def _():
        late_ref[3] = dy_ref[...]
        late_ref[4] = out_ref[...]


def exchange_kernel(side, halves, early_ref, late_ref, *refs):
    own_outs, other_outs = refs[: 2 * halves], refs[2 * halves : 4 * halves]
    early, near, far, pair_early, pair_late, total, landed, gathered = refs[4 * halves : -9]
    send_sem, recv_sem, early_sem, ring_send, ring_recv, out_sem, swap_send, swap_recv, load_sem = refs[-9:]
    me = lax.axis_index("sp")
    core, sign, at, ahead, behind, wrap = neighbours(me, side)
    partner = me + sign

    barrier = pltpu.get_barrier_semaphore()
    for other in ahead + behind + (partner,):
        pl.semaphore_signal(barrier, inc=1, device_id={"sp": other}, device_id_type=MESH)
    pl.semaphore_wait(barrier, 5)

    half = early_ref.shape[3]
    block = half // N_CORES

    def send(*args):
        copy = remote(*args)
        copy.start()
        return copy

    def late_of(which, part):
        return late_ref.at[which + part * (which // (N_GRADS - 1))]

    copies = {}

    def start(part, kind, src, dst, target):
        copies[part, kind] = send(src, dst, send_sem.at[part, kind], recv_sem.at[part, kind], target)

    for part in range(2):
        start(part, 3, late_of(wrap(at[part] + 2), part), far.at[part], ahead[part])
    for part in range(2):
        start(part, 1, late_of(wrap(at[part] - sign), part), near.at[part, 1], behind[part])
        start(part, 7, late_of(at[part], part), pair_late.at[part, 3], partner)
    for part in range(2):
        start(part, 0, late_of(wrap(at[part] + sign), part), near.at[part, 0], ahead[part])
    load = pltpu.make_async_copy(early_ref, early, load_sem.at[0])
    load.start()
    shares = [send(early_ref.at[part], pair_early.at[part], early_sem.at[0, part], early_sem.at[1, part], partner) for part in range(2)]

    n_tiles = 2
    width = half // n_tiles

    def my_cols(start):
        return pl.ds(pl.multiple_of(start + core * block, block), block)

    def accumulate(part, early_part, late_part, fresh=False):
        def add(left_value, right, offset, right_offset):
            def tile(t, carry):
                cols = pl.ds(pl.multiple_of(offset + t * width, width), width)
                product = dot(left_value, right[:, pl.ds(pl.multiple_of(right_offset + t * width, width), width)], (0, 0))
                if fresh:
                    total[part, :, cols] = product
                else:
                    total[part, :, cols] += product
                return carry

            return tile

        @pl.when(at[part] < N_GRADS - 1)
        def _():
            lax.fori_loop(0, 2 * n_tiles, add(early_part[:, my_cols(0)], late_part, 0, 0), 0)

        @pl.when(at[part] == N_GRADS - 1)
        def _():
            left_value = late_part[:, my_cols(part * half)]
            lax.fori_loop(0, n_tiles, add(left_value, early_part, part * half, 0), 0)
            lax.fori_loop(0, n_tiles, add(left_value, late_part, (1 - part) * half, (1 - part) * half), 0)

    def take(part, slot):
        copies[part, slot].wait_recv()
        start(part, 4 + slot, near.at[part, slot], pair_late.at[part, slot], partner)
        accumulate(part, early.at[part, slot], near.at[part, slot])

    def take_other(part, slot):
        copies[part, 4 + slot].wait_recv()
        accumulate(part, pair_early.at[part, slot], pair_late.at[part, slot])

    load.wait()
    for part in range(2):
        accumulate(part, early.at[part, 3], late_of(at[part], part), fresh=True)
    for part in range(2):
        shares[part].wait_recv()
        take_other(part, 3)
    for part in range(2):
        copies[part, 3].wait_recv()
        start(part, 2, far.at[part], near.at[part, 2], ahead[part])
    for slot in (1, 0, 2):
        for part in range(2):
            take(part, slot)
        for part in range(2):
            take_other(part, slot)

    piece = block // side
    small = piece // halves

    def rows(part, shift, h):
        return pl.ds(pl.multiple_of(wrap(at[1 - part] + sign * shift) * piece + h * small, small), small)

    def ring(part, h, step, src, dst):
        return send(src, dst, ring_send.at[part, h, step], ring_recv.at[part, h, step], ahead[1 - part])

    lanes = [(part, h) for h in range(halves) for part in range(2)]
    hops = {}
    for part, h in lanes:
        hops[part, h, 0] = ring(part, h, 0, total.at[part, rows(part, -1, h)], landed.at[part, h, 0])
    for step in range(1, side - 1):
        for part, h in lanes:
            hops[part, h, step - 1].wait_recv()
            landed[part, h, step - 1] += total[part, rows(part, -(step + 1), h), :]
            hops[part, h, step] = ring(part, h, step, landed.at[part, h, step - 1], landed.at[part, h, step])
    stores = []

    swaps = []

    def store(part, h, shift, n):
        src = gathered.at[part, rows(part, shift, h)]
        where = pl.ds(pl.multiple_of(wrap(at[1 - part] + sign * shift) * small, small), small)
        copy = pltpu.make_async_copy(src, own_outs[2 * h + part].at[where], out_sem.at[part, h, n])
        copy.start()
        stores.append(copy)
        swaps.append(send(src, other_outs[2 * h + part].at[where], swap_send.at[part, h, n], swap_recv.at[part, h, n], partner))

    last = side - 1
    for part, h in lanes:
        hops[part, h, last - 1].wait_recv()
        mine = rows(part, 0, h)
        gathered[part, mine, :] = landed[part, h, last - 1] + total[part, mine, :]
        hops[part, h, last] = ring(part, h, last, gathered.at[part, mine], gathered.at[part, mine])
        store(part, h, 0, 0)
    for step in range(1, side):
        for part, h in lanes:
            hops[part, h, last + step - 1].wait_recv()
            where = rows(part, -step, h)
            if step < side - 1:
                hops[part, h, last + step] = ring(part, h, last + step, gathered.at[part, where], gathered.at[part, where])
            store(part, h, -step, step)
    for copy in stores:
        copy.wait()
    for copy in list(copies.values()) + shares:
        copy.wait_send()
    for copy in hops.values():
        copy.wait_send()
    for copy in swaps:
        copy.wait()


def place_kernel(side, step, lane, halves, fresh, *refs):
    blocks = refs[:4]
    grads = refs[4 if fresh else 4 + N_GRADS :][:N_GRADS]
    buf, sem_in, sem_out = refs[-3:]
    index = lax.axis_index("sp")
    core = lax.rem(index, N_CORES)
    col = lax.rem(index // N_CORES, side)
    row = index // (N_CORES * side)
    small = blocks[0].shape[0] // side
    piece = small * halves
    half = grads[0].shape[0] // 2
    jobs = []
    for k, src in enumerate(blocks):
        own, part = k < 2, k % 2
        at = col if part == 0 else row
        c = core if own else 1 - core
        which = lax.rem(at - (1 - 2 * c) * step + 2 * side, side)
        start = part * half + c * side * piece + lane * small
        for g in range(side):
            jobs.append((src.at[pl.ds(g * small, small)], which, pl.multiple_of(start + g * piece, small)))
    for n, (src, which, start) in enumerate(jobs):
        pltpu.make_async_copy(src, buf.at[n], sem_in.at[n]).start()
    for n, (src, which, start) in enumerate(jobs):
        pltpu.make_async_copy(src, buf.at[n], sem_in.at[n]).wait()
        for m in range(N_GRADS):

            @pl.when(which == m)
            def _():
                pltpu.make_async_copy(buf.at[n], grads[m].at[pl.ds(start, small)], sem_out.at[n]).start()

    for n, (src, which, start) in enumerate(jobs):
        pltpu.make_async_copy(buf.at[n], grads[0].at[pl.ds(0, small)], sem_out.at[n]).wait()


def solution(mesh):
    n_seq = mesh.shape["sp"]
    side = math.isqrt(n_seq // N_CORES)
    row_spec = P(("dp", "sp"), None)
    grad_spec = P("dp", None)

    def device_at(row, col, core):
        return ((row % side) * side + col % side) * N_CORES + core

    def ring_perm(axis, hops):
        pairs = []
        for row in range(side):
            for col in range(side):
                for core in range(N_CORES):
                    shift = hops * (1 - 2 * core)
                    target = device_at(row, col + shift, core) if axis == "x" else device_at(row + shift, col, core)
                    pairs.append((device_at(row, col, core), target))
        return pairs

    core_perm = [(j, j ^ 1) for j in range(n_seq)]

    def local_layer(tokens, w_q, w_k, w_v, w_o, grad_y):
        n_rows, model_dim = tokens.shape
        n_heads = model_dim // HEAD_DIM
        att_scale = 1.0 / math.sqrt(n_rows * n_seq * HEAD_DIM)
        index = lax.axis_index("sp")
        core = lax.rem(index, N_CORES)
        place = {"x": lax.rem(index // N_CORES, side), "y": index // (N_CORES * side)}

        def swap_cores(value):
            return lax.ppermute(value, "sp", perm=core_perm)

        def hop(value, axis, hops):
            return lax.ppermute(value, "sp", perm=ring_perm(axis, hops))

        def project(operand, weight):
            return jnp.dot(operand, weight, preferred_element_type=F32).astype(BF16)

        def back_proj(rows, weight):
            return jnp.einsum("ne,de->nd", rows, weight, preferred_element_type=F32)

        tile = 2 * HEAD_DIM
        state_shape = (2, n_heads, HEAD_DIM, HEAD_DIM)
        full = pl.BlockSpec((n_rows, model_dim), lambda i: (0, 0))
        in_cols = pl.BlockSpec((model_dim, tile), lambda i: (0, i))
        in_rows = pl.BlockSpec((tile, model_dim), lambda i: (i, 0))
        out_cols = pl.BlockSpec((n_rows, tile), lambda i: (0, i))
        act = jax.ShapeDtypeStruct((n_rows, model_dim), BF16)
        half = model_dim // 2
        dma = pltpu.SemaphoreType.DMA
        anywhere = pl.BlockSpec(memory_space=pl.ANY)
        n_group = n_heads // N_CORES
        q, k, v, do, early, states = pl.pallas_call(
            functools.partial(project_kernel, side),
            grid=(model_dim // tile,),
            in_specs=[full, full, in_cols, in_cols, in_cols, in_rows, anywhere, anywhere],
            out_specs=[out_cols] * 4 + [anywhere] * 2,
            out_shape=[act] * 4 + [jax.ShapeDtypeStruct((2, 4, n_rows, half), BF16), jax.ShapeDtypeStruct(state_shape, F32)],
            scratch_shapes=[VMEM(state_shape, F32)] * 2
            + [VMEM((2, n_rows, half), BF16), dma((2, 4)), dma((2, 4)), dma((3,))]
            + [VMEM((2, n_group, HEAD_DIM, HEAD_DIM), F32)] * 6
            + [dma((2,))] * 2
            + [dma((2, n_group))] * 4
            + [dma((2, n_group, side - 1))]
            + [dma((2, n_group))] * 2,
            cost_estimate=pl.CostEstimate(flops=8 * n_rows * model_dim * model_dim, bytes_accessed=8 * model_dim * model_dim, transcendentals=0),
            compiler_params=pltpu.CompilerParams(collective_id=3, has_side_effects=True, vmem_limit_bytes=48 * 2**20),
            name="project",
        )(tokens, grad_y, w_q, w_k, w_v, w_o, tokens, grad_y)

        head_cols = pl.BlockSpec((n_rows, HEAD_DIM), lambda h: (0, h))
        out_rows, late = pl.pallas_call(
            functools.partial(attend_kernel, att_scale),
            grid=(n_heads,),
            in_specs=[head_cols] * 5 + [pl.BlockSpec((2, 1, HEAD_DIM, HEAD_DIM), lambda h: (0, h, 0, 0))],
            out_specs=[head_cols, pl.BlockSpec((5, n_rows, HEAD_DIM), lambda h: (0, 0, h))],
            out_shape=[act, jax.ShapeDtypeStruct((5, n_rows, model_dim), BF16)],
            cost_estimate=pl.CostEstimate(flops=n_heads * 24 * 2 * 128**3, bytes_accessed=2**24, transcendentals=0),
            compiler_params=pltpu.CompilerParams(vmem_limit_bytes=16 * 2**20),
            name="attend",
        )(q, k, v, do, grad_y, states)

        block = half // N_CORES
        halves = 2
        small = block // side // halves
        axes = (("x", "y"), ("y", "x"))
        blocks = pl.pallas_call(
            functools.partial(exchange_kernel, side, halves),
            in_specs=[anywhere, pl.BlockSpec(memory_space=VMEM)],
            out_specs=[anywhere] * (4 * halves),
            out_shape=[jax.ShapeDtypeStruct((block // halves, model_dim), F32)] * (4 * halves),
            scratch_shapes=[
                VMEM((2, 4, n_rows, half), BF16),
                VMEM((2, 3, n_rows, model_dim), BF16),
                VMEM((2, n_rows, model_dim), BF16),
                VMEM((2, 4, n_rows, half), BF16),
                VMEM((2, 4, n_rows, model_dim), BF16),
                VMEM((2, block, model_dim), F32),
                VMEM((2, halves, side - 1, small, model_dim), F32),
                VMEM((2, block, model_dim), F32),
                dma((2, 8)),
                dma((2, 8)),
                dma((2, 2)),
                dma((2, halves, 2 * (side - 1))),
                dma((2, halves, 2 * (side - 1))),
                dma((2, halves, side)),
                dma((2, halves, side)),
                dma((2, halves, side)),
                dma((1,)),
            ],
            cost_estimate=pl.CostEstimate(flops=2 * 2 * block * model_dim * n_rows * 8, bytes_accessed=2**24, transcendentals=0),
            compiler_params=pltpu.CompilerParams(collective_id=1, has_side_effects=True, vmem_limit_bytes=60 * 2**20),
            name="exchange",
        )(early, late)
        own = [list(blocks[2 * h : 2 * h + 2]) for h in range(halves)]
        others = [list(blocks[2 * (halves + h) : 2 * (halves + h) + 2]) for h in range(halves)]

        grads = []
        n_copies = 4 * side
        for step in range(side):
            for h in range(halves):
                if step:
                    for part, (first, second) in enumerate(axes):
                        own[h][part] = hop(own[h][part], first, 1)
                    others[h] = [swap_cores(b) for b in own[h]]
                fresh = not grads
                place_blocks = pl.pallas_call(
                    functools.partial(place_kernel, side, step, h, halves, fresh),
                    in_specs=[pl.BlockSpec(memory_space=pl.ANY)] * (4 + len(grads)),
                    out_specs=[pl.BlockSpec(memory_space=pl.ANY)] * N_GRADS,
                    out_shape=[jax.ShapeDtypeStruct((model_dim, model_dim), F32)] * N_GRADS,
                    scratch_shapes=[VMEM((n_copies, small, model_dim), F32), dma((n_copies,)), dma((n_copies,))],
                    input_output_aliases={} if fresh else {4 + m: m for m in range(N_GRADS)},
                    cost_estimate=pl.CostEstimate(flops=3 * 10**9, bytes_accessed=32 * n_copies * small * model_dim, transcendentals=0),
                )
                grads = place_blocks(*own[h], *others[h], *grads)

        out_y = project(out_rows, w_o)
        grad_x = back_proj(late[0], w_q)
        grad_x = grad_x + back_proj(late[1], w_k)
        grad_x = (grad_x + back_proj(late[2], w_v)).astype(BF16)
        return (out_y, grad_x) + tuple(grads)

    return jax.shard_map(local_layer, mesh=mesh, in_specs=(row_spec, P(), P(), P(), P(), row_spec), out_specs=(row_spec, row_spec, grad_spec, grad_spec, grad_spec, grad_spec), check_vma=False)
```

```python
import functools
import math
import jax
import jax.numpy as jnp
from jax import lax
from jax.experimental import pallas as pl
from jax.experimental.pallas import tpu as pltpu
from jax.sharding import PartitionSpec as P


HEAD_DIM = 128
BLOCK_LEN = 128
N_CORES = 2
N_GRADS = 4
RELAY_STEP = 7
SLOTS = 3


F32 = jnp.float32
BF16 = jnp.bfloat16
VMEM = pltpu.VMEM
MESH = pl.DeviceIdType.MESH


def dot(a, b, dims):
    return lax.dot_general(a, b, ((dims[:1], dims[1:]), ((), ())), preferred_element_type=F32)


def neighbours(me, side):
    core = lax.rem(me, N_CORES)
    sign = 1 - 2 * core
    col = lax.rem(me // N_CORES, side)
    row = me // (N_CORES * side)

    def wrap(value):
        return lax.rem(value + 2 * side, side)

    def device(r, c):
        return (r * side + c) * N_CORES + core

    ahead = (device(row, wrap(col + sign)), device(wrap(row + sign), col))
    behind = (device(row, wrap(col - sign)), device(wrap(row - sign), col))
    return core, sign, (col, row), ahead, behind, wrap


def remote(src, dst, send, recv, target):
    return pltpu.make_async_remote_copy(src_ref=src, dst_ref=dst, send_sem=send, recv_sem=recv, device_id={"sp": target}, device_id_type=MESH)


def chain(side, totals_ref, out_ref, other, before, stage, above, down, peer, swap_send, swap_recv, row_send, row_recv, above_recv, down_send, cast_send, back_send, back_recv):
    me = lax.axis_index("sp")
    core = lax.rem(me, N_CORES)
    col = lax.rem(me // N_CORES, side)
    row = me // (N_CORES * side)
    partner = me + 1 - 2 * core
    n_group = totals_ref.shape[1] // N_CORES
    mine, yours = core * n_group, (1 - core) * n_group

    def wrap(value):
        return lax.rem(value + 2 * side, side)

    def device(r, c):
        return (wrap(r) * side + wrap(c)) * N_CORES + core

    def copy(src, dst, send, recv, target):
        return pltpu.make_async_remote_copy(src_ref=src, dst_ref=dst, send_sem=send, recv_sem=recv, device_id={"sp": target}, device_id_type=MESH)

    def swap_copy(kind):
        return copy(totals_ref.at[kind, pl.ds(yours, n_group)], other.at[kind], swap_send.at[kind], swap_recv.at[kind], partner)

    def row_copy(kind, h):
        return copy(stage.at[kind, h], before.at[kind, h], row_send.at[kind, h], row_recv.at[kind, h], device(row, col + 1 - 2 * kind))

    def down_copy(kind, h):
        return copy(down.at[kind, h], above.at[kind, h], down_send.at[kind, h], above_recv.at[kind, h], device(row + 1 - 2 * kind, col))

    def cast_copy(kind, h, t):
        return copy(above.at[kind, h], above.at[kind, h], cast_send.at[kind, h, t - 1], above_recv.at[kind, h], device(row, col + t))

    def back_copy(kind, h):
        return copy(peer.at[kind, h], out_ref.at[kind, mine + h], back_send.at[kind, h], back_recv.at[kind, h], partner)

    def position(kind, coordinate):
        return kind * (side - 1) + (1 - 2 * kind) * coordinate

    for kind in range(2):
        swap_copy(kind).start()
    for kind in range(2):

        @pl.when(position(kind, col) == 0)
        def _():
            before[kind] = jnp.zeros_like(before[kind])

        @pl.when((position(kind, col) == side - 1) & (position(kind, row) == 0))
        def _():
            above[kind] = jnp.zeros_like(above[kind])

    for kind in range(2):
        swap_copy(kind).wait()

    def run(slot, carry):
        for kind in range(2):
            along, across = position(kind, col), position(kind, row)
            h = slot - SLOTS * along

            @pl.when((h >= 0) & (h < n_group))
            def _():
                @pl.when(along > 0)
                def _():
                    row_copy(kind, h).wait_recv()

                stage[kind, h] = before[kind, h] + (totals_ref[kind, mine + h] + other[kind, h])

                @pl.when(along < side - 1)
                def _():
                    row_copy(kind, h).start()

            g = slot - SLOTS * (side - 1 + across)

            @pl.when((along == side - 1) & (g >= 0) & (g < n_group))
            def _():
                @pl.when(across > 0)
                def _():
                    down_copy(kind, g).wait_recv()

                @pl.when(across < side - 1)
                def _():
                    down[kind, g] = above[kind, g] + stage[kind, g]
                    down_copy(kind, g).start()

                for t in range(1, side):
                    cast_copy(kind, g, t).start()

        return carry

    lax.fori_loop(0, 2 * SLOTS * (side - 1) + n_group, run, 0)

    def finish(h, carry):
        for kind in range(2):

            @pl.when(position(kind, col) < side - 1)
            def _():
                down_copy(kind, h).wait_recv()

            base = above[kind, h] + before[kind, h]
            own_total, other_total = totals_ref[kind, mine + h], other[kind, h]
            out_ref[kind, mine + h] = jnp.where(core == kind, base, base + other_total)
            peer[kind, h] = jnp.where(core == kind, base + own_total, base)
            back_copy(kind, h).start()
        return carry

    lax.fori_loop(0, n_group, finish, 0)

    def drain(h, carry):
        for kind in range(2):
            along, across = position(kind, col), position(kind, row)
            back_copy(kind, h).wait()

            @pl.when(along < side - 1)
            def _():
                row_copy(kind, h).wait_send()

            @pl.when(along == side - 1)
            def _():
                for t in range(1, side):
                    cast_copy(kind, h, t).wait_send()

                @pl.when(across < side - 1)
                def _():
                    down_copy(kind, h).wait_send()

        return carry

    lax.fori_loop(0, n_group, drain, 0)


def project_kernel(side, x_ref, dy_ref, wq_ref, wk_ref, wv_ref, wo_ref, x_any, dy_any, q_ref, k_ref, v_ref, do_ref, early_ref, states_ref, totals, states, relay, send_sem, recv_sem, own_sem, *chain_refs):
    core, sign, at, ahead, behind, wrap = neighbours(lax.axis_index("sp"), side)
    half = early_ref.shape[3]
    step = pl.program_id(0)

    def early(part, kind, src):
        dst = relay.at[part] if kind == 3 else early_ref.at[part, kind]
        return remote(src, dst, send_sem.at[part, kind], recv_sem.at[part, kind], behind[part] if kind == 1 else ahead[part])

    def source(part, array):
        return array.at[:, pl.ds(part * half, half)]

    def start_to(part, kind, which):
        @pl.when(which < N_GRADS - 1)
        def _():
            early(part, kind, source(part, x_any)).start()

        @pl.when(which == N_GRADS - 1)
        def _():
            early(part, kind, source(part, dy_any)).start()

    def own(part, array):
        return pltpu.make_async_copy(source(part, array), early_ref.at[part, 3], own_sem.at[part])

    @pl.when(step == 0)
    def _():
        barrier = pltpu.get_barrier_semaphore()
        me = lax.axis_index("sp")
        first_in_row = at[1] * side * N_CORES + core
        peers = [first_in_row + wrap(at[0] + t) * N_CORES for t in range(1, side)] + [ahead[1], behind[1], me + sign]
        for target in peers:
            pl.semaphore_signal(barrier, inc=1, device_id={"sp": target}, device_id_type=MESH)
        pl.semaphore_wait(barrier, len(peers))
        for part in range(2):
            start_to(part, 3, wrap(at[part] + 2))
        for part in range(2):
            start_to(part, 1, wrap(at[part] - sign))
        for part in range(2):
            start_to(part, 0, wrap(at[part] + sign))

            @pl.when(at[part] < N_GRADS - 1)
            def _():
                own(part, x_any).start()

            @pl.when(at[part] == N_GRADS - 1)
            def _():
                own(part, dy_any).start()

    @pl.when(step == RELAY_STEP)
    def _():
        for part in range(2):
            early(part, 3, source(part, x_any)).wait_recv()
            early(part, 2, relay.at[part]).start()

    x = x_ref[...]
    q_ref[...] = dot(x, wq_ref[...], (1, 0)).astype(BF16)
    k_ref[...] = dot(x, wk_ref[...], (1, 0)).astype(BF16)
    v_ref[...] = dot(x, wv_ref[...], (1, 0)).astype(BF16)
    do_ref[...] = dot(dy_ref[...], wo_ref[...], (1, 1)).astype(BF16)
    for head in range(q_ref.shape[1] // HEAD_DIM):
        cols = slice(head * HEAD_DIM, (head + 1) * HEAD_DIM)
        kv = dot(k_ref[:, cols], v_ref[:, cols], (0, 0))
        qdo = dot(q_ref[:, cols], do_ref[:, cols], (0, 0))
        at_head = step * (q_ref.shape[1] // HEAD_DIM) + head
        totals[0, at_head] = kv
        totals[1, at_head] = qdo

    @pl.when(step == pl.num_programs(0) - 1)
    def _():
        chain(side, totals, states, *chain_refs)
        result = pltpu.make_async_copy(states, states_ref, own_sem.at[2])
        result.start()
        result.wait()
        for part in range(2):
            own(part, x_any).wait()
            for kind in range(4):
                copy = early(part, kind, source(part, x_any))
                copy.wait_send()
                if kind != 3:
                    copy.wait_recv()


def attend_kernel(scale, q_ref, k_ref, v_ref, do_ref, dy_ref, state_ref, out_ref, late_ref):
    n_blocks = q_ref.shape[0] // BLOCK_LEN
    rows = [pl.ds(b * BLOCK_LEN, BLOCK_LEN) for b in range(n_blocks)]
    shape = (BLOCK_LEN, BLOCK_LEN)
    causal = lax.broadcasted_iota(jnp.int32, shape, 0) >= lax.broadcasted_iota(jnp.int32, shape, 1)
    work = []
    for head in range(state_ref.shape[1]):
        cols = pl.ds(head * HEAD_DIM, HEAD_DIM)
        fwd = [state_ref[0, head]]
        for b in range(n_blocks - 1):
            fwd.append(fwd[-1] + dot(k_ref[rows[b], cols], v_ref[rows[b], cols], (0, 0)))
        rev = [state_ref[1, head]]
        for b in range(n_blocks - 1, 0, -1):
            rev.insert(0, rev[0] + dot(q_ref[rows[b], cols], do_ref[rows[b], cols], (0, 0)))
        work += [(rows[b], cols, fwd[b].astype(BF16), rev[b].astype(BF16)) for b in range(n_blocks)]
    scores = []
    for at, cols, s, r in work:
        att = jnp.where(causal, dot(q_ref[at, cols], k_ref[at, cols], (1, 1)), 0.0).astype(BF16)
        d_att = jnp.where(causal, dot(do_ref[at, cols], v_ref[at, cols], (1, 1)), 0.0).astype(BF16)
        scores.append((att, d_att))
    for (at, cols, s, r), (att, d_att) in zip(work, scores):
        q, k, v, do = q_ref[at, cols], k_ref[at, cols], v_ref[at, cols], do_ref[at, cols]
        out_ref[at, cols] = ((dot(att, v, (1, 0)) + dot(q, s, (1, 0))) * scale).astype(BF16)
        late_ref[0, at, cols] = ((dot(d_att, k, (1, 0)) + dot(do, s, (1, 1))) * scale).astype(BF16)
        late_ref[1, at, cols] = ((dot(d_att, q, (0, 0)) + dot(v, r, (1, 1))) * scale).astype(BF16)
        late_ref[2, at, cols] = ((dot(att, do, (0, 0)) + dot(k, r, (1, 0))) * scale).astype(BF16)
    first_half = pl.program_id(0) < pl.num_programs(0) // 2

    @pl.when(first_half)
    def _():
        late_ref[3] = out_ref[...]
        late_ref[4] = dy_ref[...]

    @pl.when(jnp.logical_not(first_half))
    def _():
        late_ref[3] = dy_ref[...]
        late_ref[4] = out_ref[...]


def exchange_kernel(side, halves, early_ref, late_ref, *refs):
    own_outs, other_outs = refs[: 2 * halves], refs[2 * halves : 4 * halves]
    early, near, far, pair_early, pair_late, total, landed, gathered = refs[4 * halves : -9]
    send_sem, recv_sem, early_sem, ring_send, ring_recv, out_sem, swap_send, swap_recv, load_sem = refs[-9:]
    me = lax.axis_index("sp")
    core, sign, at, ahead, behind, wrap = neighbours(me, side)
    partner = me + sign

    barrier = pltpu.get_barrier_semaphore()
    for other in ahead + behind + (partner,):
        pl.semaphore_signal(barrier, inc=1, device_id={"sp": other}, device_id_type=MESH)
    pl.semaphore_wait(barrier, 5)

    half = early_ref.shape[3]
    block = half // N_CORES

    def send(*args):
        copy = remote(*args)
        copy.start()
        return copy

    def late_of(which, part):
        return late_ref.at[which + part * (which // (N_GRADS - 1))]

    copies = {}

    def start(part, kind, src, dst, target):
        copies[part, kind] = send(src, dst, send_sem.at[part, kind], recv_sem.at[part, kind], target)

    for part in range(2):
        start(part, 3, late_of(wrap(at[part] + 2), part), far.at[part], ahead[part])
    for part in range(2):
        start(part, 1, late_of(wrap(at[part] - sign), part), near.at[part, 1], behind[part])
        start(part, 7, late_of(at[part], part), pair_late.at[part, 3], partner)
    for part in range(2):
        start(part, 0, late_of(wrap(at[part] + sign), part), near.at[part, 0], ahead[part])
    load = pltpu.make_async_copy(early_ref, early, load_sem.at[0])
    load.start()
    shares = [send(early_ref.at[part], pair_early.at[part], early_sem.at[0, part], early_sem.at[1, part], partner) for part in range(2)]

    n_tiles = 2
    width = half // n_tiles

    def my_cols(start):
        return pl.ds(pl.multiple_of(start + core * block, block), block)

    def accumulate(part, early_part, late_part, fresh=False):
        def add(left_value, right, offset, right_offset):
            def tile(t, carry):
                cols = pl.ds(pl.multiple_of(offset + t * width, width), width)
                product = dot(left_value, right[:, pl.ds(pl.multiple_of(right_offset + t * width, width), width)], (0, 0))
                if fresh:
                    total[part, :, cols] = product
                else:
                    total[part, :, cols] += product
                return carry

            return tile

        @pl.when(at[part] < N_GRADS - 1)
        def _():
            lax.fori_loop(0, 2 * n_tiles, add(early_part[:, my_cols(0)], late_part, 0, 0), 0)

        @pl.when(at[part] == N_GRADS - 1)
        def _():
            left_value = late_part[:, my_cols(part * half)]
            lax.fori_loop(0, n_tiles, add(left_value, early_part, part * half, 0), 0)
            lax.fori_loop(0, n_tiles, add(left_value, late_part, (1 - part) * half, (1 - part) * half), 0)

    def take(part, slot):
        copies[part, slot].wait_recv()
        start(part, 4 + slot, near.at[part, slot], pair_late.at[part, slot], partner)
        accumulate(part, early.at[part, slot], near.at[part, slot])

    def take_other(part, slot):
        copies[part, 4 + slot].wait_recv()
        accumulate(part, pair_early.at[part, slot], pair_late.at[part, slot])

    load.wait()
    for part in range(2):
        accumulate(part, early.at[part, 3], late_of(at[part], part), fresh=True)
    for part in range(2):
        shares[part].wait_recv()
        take_other(part, 3)
    for part in range(2):
        copies[part, 3].wait_recv()
        start(part, 2, far.at[part], near.at[part, 2], ahead[part])
    for slot in (1, 0, 2):
        for part in range(2):
            take(part, slot)
        for part in range(2):
            take_other(part, slot)

    piece = block // side
    small = piece // halves

    def rows(part, shift, h):
        return pl.ds(pl.multiple_of(wrap(at[1 - part] + sign * shift) * piece + h * small, small), small)

    def ring(part, h, step, src, dst):
        return send(src, dst, ring_send.at[part, h, step], ring_recv.at[part, h, step], ahead[1 - part])

    lanes = [(part, h) for h in range(halves) for part in range(2)]
    hops = {}
    for part, h in lanes:
        hops[part, h, 0] = ring(part, h, 0, total.at[part, rows(part, -1, h)], landed.at[part, h, 0])
    for step in range(1, side - 1):
        for part, h in lanes:
            hops[part, h, step - 1].wait_recv()
            landed[part, h, step - 1] += total[part, rows(part, -(step + 1), h), :]
            hops[part, h, step] = ring(part, h, step, landed.at[part, h, step - 1], landed.at[part, h, step])
    stores = []

    swaps = []

    def store(part, h, shift, n):
        src = gathered.at[part, rows(part, shift, h)]
        where = pl.ds(pl.multiple_of(wrap(at[1 - part] + sign * shift) * small, small), small)
        copy = pltpu.make_async_copy(src, own_outs[2 * h + part].at[where], out_sem.at[part, h, n])
        copy.start()
        stores.append(copy)
        swaps.append(send(src, other_outs[2 * h + part].at[where], swap_send.at[part, h, n], swap_recv.at[part, h, n], partner))

    last = side - 1
    for part, h in lanes:
        hops[part, h, last - 1].wait_recv()
        mine = rows(part, 0, h)
        gathered[part, mine, :] = landed[part, h, last - 1] + total[part, mine, :]
        hops[part, h, last] = ring(part, h, last, gathered.at[part, mine], gathered.at[part, mine])
        store(part, h, 0, 0)
    for step in range(1, side):
        for part, h in lanes:
            hops[part, h, last + step - 1].wait_recv()
            where = rows(part, -step, h)
            if step < side - 1:
                hops[part, h, last + step] = ring(part, h, last + step, gathered.at[part, where], gathered.at[part, where])
            store(part, h, -step, step)
    for copy in stores:
        copy.wait()
    for copy in list(copies.values()) + shares:
        copy.wait_send()
    for copy in hops.values():
        copy.wait_send()
    for copy in swaps:
        copy.wait()


def place_kernel(side, step, lane, halves, kinds, fresh, *refs):
    n_blocks = len(kinds)
    blocks = refs[:n_blocks]
    grads = refs[n_blocks if fresh else n_blocks + N_GRADS :][:N_GRADS]
    buf, sem_in, sem_out = refs[-3:]
    index = lax.axis_index("sp")
    core = lax.rem(index, N_CORES)
    col = lax.rem(index // N_CORES, side)
    row = index // (N_CORES * side)
    small = blocks[0].shape[0] // side
    piece = small * halves
    half = grads[0].shape[0] // 2
    jobs = []
    for (own, part), src in zip(kinds, blocks):
        at = col if part == 0 else row
        c = core if own else 1 - core
        which = lax.rem(at - (1 - 2 * c) * step + 2 * side, side)
        start = part * half + c * side * piece + lane * small
        for g in range(side):
            jobs.append((src.at[pl.ds(g * small, small)], which, pl.multiple_of(start + g * piece, small)))
    for n, (src, which, start) in enumerate(jobs):
        pltpu.make_async_copy(src, buf.at[n], sem_in.at[n]).start()
    for n, (src, which, start) in enumerate(jobs):
        pltpu.make_async_copy(src, buf.at[n], sem_in.at[n]).wait()
        for m in range(N_GRADS):

            @pl.when(which == m)
            def _():
                pltpu.make_async_copy(buf.at[n], grads[m].at[pl.ds(start, small)], sem_out.at[n]).start()

    for n, (src, which, start) in enumerate(jobs):
        pltpu.make_async_copy(buf.at[n], grads[0].at[pl.ds(0, small)], sem_out.at[n]).wait()


def solution(mesh):
    n_seq = mesh.shape["sp"]
    side = math.isqrt(n_seq // N_CORES)
    row_spec = P(("dp", "sp"), None)
    grad_spec = P("dp", None)

    def device_at(row, col, core):
        return ((row % side) * side + col % side) * N_CORES + core

    def ring_perm(axis, hops):
        pairs = []
        for row in range(side):
            for col in range(side):
                for core in range(N_CORES):
                    shift = hops * (1 - 2 * core)
                    target = device_at(row, col + shift, core) if axis == "x" else device_at(row + shift, col, core)
                    pairs.append((device_at(row, col, core), target))
        return pairs

    core_perm = [(j, j ^ 1) for j in range(n_seq)]

    def local_layer(tokens, w_q, w_k, w_v, w_o, grad_y):
        n_rows, model_dim = tokens.shape
        n_heads = model_dim // HEAD_DIM
        att_scale = 1.0 / math.sqrt(n_rows * n_seq * HEAD_DIM)
        index = lax.axis_index("sp")
        core = lax.rem(index, N_CORES)
        place = {"x": lax.rem(index // N_CORES, side), "y": index // (N_CORES * side)}

        def swap_cores(value):
            return lax.ppermute(value, "sp", perm=core_perm)

        def hop(value, axis, hops):
            return lax.ppermute(value, "sp", perm=ring_perm(axis, hops))

        def project(operand, weight):
            return jnp.dot(operand, weight, preferred_element_type=F32).astype(BF16)

        def back_proj(rows, weight):
            return jnp.einsum("ne,de->nd", rows, weight, preferred_element_type=F32)

        tile = 2 * HEAD_DIM
        state_shape = (2, n_heads, HEAD_DIM, HEAD_DIM)
        full = pl.BlockSpec((n_rows, model_dim), lambda i: (0, 0))
        in_cols = pl.BlockSpec((model_dim, tile), lambda i: (0, i))
        in_rows = pl.BlockSpec((tile, model_dim), lambda i: (i, 0))
        out_cols = pl.BlockSpec((n_rows, tile), lambda i: (0, i))
        act = jax.ShapeDtypeStruct((n_rows, model_dim), BF16)
        half = model_dim // 2
        dma = pltpu.SemaphoreType.DMA
        anywhere = pl.BlockSpec(memory_space=pl.ANY)
        n_group = n_heads // N_CORES
        q, k, v, do, early, states = pl.pallas_call(
            functools.partial(project_kernel, side),
            grid=(model_dim // tile,),
            in_specs=[full, full, in_cols, in_cols, in_cols, in_rows, anywhere, anywhere],
            out_specs=[out_cols] * 4 + [anywhere] * 2,
            out_shape=[act] * 4 + [jax.ShapeDtypeStruct((2, 4, n_rows, half), BF16), jax.ShapeDtypeStruct(state_shape, F32)],
            scratch_shapes=[VMEM(state_shape, F32)] * 2
            + [VMEM((2, n_rows, half), BF16), dma((2, 4)), dma((2, 4)), dma((3,))]
            + [VMEM((2, n_group, HEAD_DIM, HEAD_DIM), F32)] * 6
            + [dma((2,))] * 2
            + [dma((2, n_group))] * 4
            + [dma((2, n_group, side - 1))]
            + [dma((2, n_group))] * 2,
            cost_estimate=pl.CostEstimate(flops=8 * n_rows * model_dim * model_dim, bytes_accessed=8 * model_dim * model_dim, transcendentals=0),
            compiler_params=pltpu.CompilerParams(collective_id=3, has_side_effects=True, vmem_limit_bytes=48 * 2**20),
            name="project",
        )(tokens, grad_y, w_q, w_k, w_v, w_o, tokens, grad_y)

        out_rows, late = pl.pallas_call(
            functools.partial(attend_kernel, att_scale),
            grid=(model_dim // tile,),
            in_specs=[out_cols] * 5 + [pl.BlockSpec((2, tile // HEAD_DIM, HEAD_DIM, HEAD_DIM), lambda i: (0, i, 0, 0))],
            out_specs=[out_cols, pl.BlockSpec((5, n_rows, tile), lambda i: (0, 0, i))],
            out_shape=[act, jax.ShapeDtypeStruct((5, n_rows, model_dim), BF16)],
            cost_estimate=pl.CostEstimate(flops=n_heads * 24 * 2 * 128**3, bytes_accessed=2**24, transcendentals=0),
            compiler_params=pltpu.CompilerParams(vmem_limit_bytes=16 * 2**20),
            name="attend",
        )(q, k, v, do, grad_y, states)

        block = half // N_CORES
        halves = 2
        small = block // side // halves
        axes = (("x", "y"), ("y", "x"))
        blocks = pl.pallas_call(
            functools.partial(exchange_kernel, side, halves),
            in_specs=[anywhere, pl.BlockSpec(memory_space=VMEM)],
            out_specs=[anywhere] * (4 * halves),
            out_shape=[jax.ShapeDtypeStruct((block // halves, model_dim), F32)] * (4 * halves),
            scratch_shapes=[
                VMEM((2, 4, n_rows, half), BF16),
                VMEM((2, 3, n_rows, model_dim), BF16),
                VMEM((2, n_rows, model_dim), BF16),
                VMEM((2, 4, n_rows, half), BF16),
                VMEM((2, 4, n_rows, model_dim), BF16),
                VMEM((2, block, model_dim), F32),
                VMEM((2, halves, side - 1, small, model_dim), F32),
                VMEM((2, block, model_dim), F32),
                dma((2, 8)),
                dma((2, 8)),
                dma((2, 2)),
                dma((2, halves, 2 * (side - 1))),
                dma((2, halves, 2 * (side - 1))),
                dma((2, halves, side)),
                dma((2, halves, side)),
                dma((2, halves, side)),
                dma((1,)),
            ],
            cost_estimate=pl.CostEstimate(flops=2 * 2 * block * model_dim * n_rows * 8, bytes_accessed=2**24, transcendentals=0),
            compiler_params=pltpu.CompilerParams(collective_id=1, has_side_effects=True, vmem_limit_bytes=60 * 2**20),
            name="exchange",
        )(early, late)
        own = [list(blocks[2 * h : 2 * h + 2]) for h in range(halves)]
        others = [list(blocks[2 * (halves + h) : 2 * (halves + h) + 2]) for h in range(halves)]

        grads = []

        def put(kinds, sources, step, h):
            n_copies = len(kinds) * side
            return pl.pallas_call(
                functools.partial(place_kernel, side, step, h, halves, kinds, not grads),
                in_specs=[anywhere] * (len(kinds) + len(grads)),
                out_specs=[anywhere] * N_GRADS,
                out_shape=[jax.ShapeDtypeStruct((model_dim, model_dim), F32)] * N_GRADS,
                scratch_shapes=[VMEM((n_copies, small, model_dim), F32), dma((n_copies,)), dma((n_copies,))],
                input_output_aliases={len(kinds) + m: m for m in range(len(grads))},
                cost_estimate=pl.CostEstimate(flops=3 * 10**9, bytes_accessed=8 * n_copies * small * model_dim, transcendentals=0),
            )(*sources, *grads)

        own_kinds, other_kinds = ((True, 0), (True, 1)), ((False, 0), (False, 1))
        for step in range(side):
            for h in range(halves):
                if step:
                    for part, (first, second) in enumerate(axes):
                        own[h][part] = hop(own[h][part], first, 1)
                    for part in range(2):
                        others[h][part] = swap_cores(own[h][part])
                if (step, h) == (side - 1, halves - 1):
                    grads = put(own_kinds, own[h], step, h)
                    grads = put(other_kinds, others[h], step, h)
                else:
                    grads = put(own_kinds + other_kinds, own[h] + others[h], step, h)

        out_y = project(out_rows, w_o)
        grad_x = back_proj(late[0], w_q)
        grad_x = grad_x + back_proj(late[1], w_k)
        grad_x = (grad_x + back_proj(late[2], w_v)).astype(BF16)
        return (out_y, grad_x) + tuple(grads)

    return jax.shard_map(local_layer, mesh=mesh, in_specs=(row_spec, P(), P(), P(), P(), row_spec), out_specs=(row_spec, row_spec, grad_spec, grad_spec, grad_spec, grad_spec), check_vma=False)
```

```python
import functools
import math
import jax
import jax.numpy as jnp
from jax import lax
from jax.experimental import pallas as pl
from jax.experimental.pallas import tpu as pltpu
from jax.sharding import PartitionSpec as P


HEAD_DIM = 128
BLOCK_LEN = 128
N_CORES = 2
N_GRADS = 4
RELAY_STEP = 7
SLOTS = 2


F32 = jnp.float32
BF16 = jnp.bfloat16
VMEM = pltpu.VMEM
MESH = pl.DeviceIdType.MESH


def dot(a, b, dims):
    return lax.dot_general(a, b, ((dims[:1], dims[1:]), ((), ())), preferred_element_type=F32)


def neighbours(me, side):
    core = lax.rem(me, N_CORES)
    sign = 1 - 2 * core
    col = lax.rem(me // N_CORES, side)
    row = me // (N_CORES * side)

    def wrap(value):
        return lax.rem(value + 2 * side, side)

    def device(r, c):
        return (r * side + c) * N_CORES + core

    ahead = (device(row, wrap(col + sign)), device(wrap(row + sign), col))
    behind = (device(row, wrap(col - sign)), device(wrap(row - sign), col))
    return core, sign, (col, row), ahead, behind, wrap


def remote(src, dst, send, recv, target):
    return pltpu.make_async_remote_copy(src_ref=src, dst_ref=dst, send_sem=send, recv_sem=recv, device_id={"sp": target}, device_id_type=MESH)


def chain(side, totals_ref, out_ref, other, before, stage, above, down, peer, swap_send, swap_recv, row_send, row_recv, above_recv, down_send, cast_send, back_send, back_recv):
    me = lax.axis_index("sp")
    core = lax.rem(me, N_CORES)
    col = lax.rem(me // N_CORES, side)
    row = me // (N_CORES * side)
    partner = me + 1 - 2 * core
    n_group = totals_ref.shape[1] // N_CORES
    mine, yours = core * n_group, (1 - core) * n_group

    def wrap(value):
        return lax.rem(value + 2 * side, side)

    def device(r, c):
        return (wrap(r) * side + wrap(c)) * N_CORES + core

    def copy(src, dst, send, recv, target):
        return pltpu.make_async_remote_copy(src_ref=src, dst_ref=dst, send_sem=send, recv_sem=recv, device_id={"sp": target}, device_id_type=MESH)

    def swap_copy(kind):
        return copy(totals_ref.at[kind, pl.ds(yours, n_group)], other.at[kind], swap_send.at[kind], swap_recv.at[kind], partner)

    def row_copy(kind, h):
        return copy(stage.at[kind, h], before.at[kind, h], row_send.at[kind, h], row_recv.at[kind, h], device(row, col + 1 - 2 * kind))

    def down_copy(kind, h):
        return copy(down.at[kind, h], above.at[kind, h], down_send.at[kind, h], above_recv.at[kind, h], device(row + 1 - 2 * kind, col))

    def cast_copy(kind, h, n):
        along = (1 - 2 * kind) * (1, -1, 1 - 2 * core)[n]
        return copy(above.at[kind, h], above.at[kind, h], cast_send.at[kind, h, n], above_recv.at[kind, h], device(row, col + along))

    def back_copy(kind, h):
        return copy(peer.at[kind, h], out_ref.at[kind, mine + h], back_send.at[kind, h], back_recv.at[kind, h], partner)

    def position(kind, coordinate):
        return kind * (side - 1) + (1 - 2 * kind) * coordinate

    for kind in range(2):
        swap_copy(kind).start()
    for kind in range(2):

        @pl.when(position(kind, col) == 0)
        def _():
            before[kind] = jnp.zeros_like(before[kind])

        @pl.when((position(kind, col) == side - 1) & (position(kind, row) == 0))
        def _():
            above[kind] = jnp.zeros_like(above[kind])

    for kind in range(2):
        swap_copy(kind).wait()

    def run(slot, carry):
        for kind in range(2):
            along, across = position(kind, col), position(kind, row)
            h = slot - SLOTS * along

            @pl.when((h >= 0) & (h < n_group))
            def _():
                @pl.when(along > 0)
                def _():
                    row_copy(kind, h).wait_recv()

                stage[kind, h] = before[kind, h] + (totals_ref[kind, mine + h] + other[kind, h])

                @pl.when(along < side - 1)
                def _():
                    row_copy(kind, h).start()

            g = slot - SLOTS * (side - 1 + across)

            @pl.when((along == side - 1) & (g >= 0) & (g < n_group))
            def _():
                @pl.when(across > 0)
                def _():
                    down_copy(kind, g).wait_recv()

                @pl.when(across < side - 1)
                def _():
                    down[kind, g] = above[kind, g] + stage[kind, g]
                    down_copy(kind, g).start()

                for n in range(2):
                    cast_copy(kind, g, n).start()

        return carry

    lax.fori_loop(0, 2 * SLOTS * (side - 1) + n_group, run, 0)

    def finish(h, carry):
        for i in range(2):
            kind = lax.rem(1 - col // (side // 2) + i, 2)
            along = position(kind, col)

            @pl.when(along < side - 1)
            def _():
                down_copy(kind, h).wait_recv()

            @pl.when(along == 2 * core)
            def _():
                cast_copy(kind, h, 2).start()

        for kind in range(2):
            base = above[kind, h] + before[kind, h]
            own_total, other_total = totals_ref[kind, mine + h], other[kind, h]
            out_ref[kind, mine + h] = jnp.where(core == kind, base, base + other_total)
            peer[kind, h] = jnp.where(core == kind, base + own_total, base)
            back_copy(kind, h).start()
        return carry

    lax.fori_loop(0, n_group, finish, 0)

    def drain(h, carry):
        for kind in range(2):
            along, across = position(kind, col), position(kind, row)
            back_copy(kind, h).wait()

            @pl.when(along == 2 * core)
            def _():
                cast_copy(kind, h, 2).wait_send()

            @pl.when(along < side - 1)
            def _():
                row_copy(kind, h).wait_send()

            @pl.when(along == side - 1)
            def _():
                for n in range(2):
                    cast_copy(kind, h, n).wait_send()

                @pl.when(across < side - 1)
                def _():
                    down_copy(kind, h).wait_send()

        return carry

    lax.fori_loop(0, n_group, drain, 0)


def project_kernel(side, x_ref, dy_ref, wq_ref, wk_ref, wv_ref, wo_ref, x_any, dy_any, q_ref, k_ref, v_ref, do_ref, early_ref, states_ref, totals, states, relay, send_sem, recv_sem, own_sem, *chain_refs):
    core, sign, at, ahead, behind, wrap = neighbours(lax.axis_index("sp"), side)
    half = early_ref.shape[3]
    step = pl.program_id(0)

    def early(part, kind, src):
        dst = relay.at[part] if kind == 3 else early_ref.at[part, kind]
        return remote(src, dst, send_sem.at[part, kind], recv_sem.at[part, kind], behind[part] if kind == 1 else ahead[part])

    def source(part, array):
        return array.at[:, pl.ds(part * half, half)]

    def start_to(part, kind, which):
        @pl.when(which < N_GRADS - 1)
        def _():
            early(part, kind, source(part, x_any)).start()

        @pl.when(which == N_GRADS - 1)
        def _():
            early(part, kind, source(part, dy_any)).start()

    def own(part, array):
        return pltpu.make_async_copy(source(part, array), early_ref.at[part, 3], own_sem.at[part])

    @pl.when(step == 0)
    def _():
        barrier = pltpu.get_barrier_semaphore()
        me = lax.axis_index("sp")
        first_in_row = at[1] * side * N_CORES + core
        peers = [first_in_row + wrap(at[0] + t) * N_CORES for t in range(1, side)] + [ahead[1], behind[1], me + sign]
        for target in peers:
            pl.semaphore_signal(barrier, inc=1, device_id={"sp": target}, device_id_type=MESH)
        pl.semaphore_wait(barrier, len(peers))
        for part in range(2):
            start_to(part, 3, wrap(at[part] + 2))
        for part in range(2):
            start_to(part, 1, wrap(at[part] - sign))
        for part in range(2):
            start_to(part, 0, wrap(at[part] + sign))

            @pl.when(at[part] < N_GRADS - 1)
            def _():
                own(part, x_any).start()

            @pl.when(at[part] == N_GRADS - 1)
            def _():
                own(part, dy_any).start()

    @pl.when(step == RELAY_STEP)
    def _():
        for part in range(2):
            early(part, 3, source(part, x_any)).wait_recv()
            early(part, 2, relay.at[part]).start()

    x = x_ref[...]
    q_ref[...] = dot(x, wq_ref[...], (1, 0)).astype(BF16)
    k_ref[...] = dot(x, wk_ref[...], (1, 0)).astype(BF16)
    v_ref[...] = dot(x, wv_ref[...], (1, 0)).astype(BF16)
    do_ref[...] = dot(dy_ref[...], wo_ref[...], (1, 1)).astype(BF16)
    for head in range(q_ref.shape[1] // HEAD_DIM):
        cols = slice(head * HEAD_DIM, (head + 1) * HEAD_DIM)
        kv = dot(k_ref[:, cols], v_ref[:, cols], (0, 0))
        qdo = dot(q_ref[:, cols], do_ref[:, cols], (0, 0))
        at_head = step * (q_ref.shape[1] // HEAD_DIM) + head
        totals[0, at_head] = kv
        totals[1, at_head] = qdo

    @pl.when(step == pl.num_programs(0) - 1)
    def _():
        chain(side, totals, states, *chain_refs)
        result = pltpu.make_async_copy(states, states_ref, own_sem.at[2])
        result.start()
        result.wait()
        for part in range(2):
            own(part, x_any).wait()
            for kind in range(4):
                copy = early(part, kind, source(part, x_any))
                copy.wait_send()
                if kind != 3:
                    copy.wait_recv()


def attend_kernel(scale, q_ref, k_ref, v_ref, do_ref, dy_ref, state_ref, out_ref, late_ref):
    n_blocks = q_ref.shape[0] // BLOCK_LEN
    rows = [pl.ds(b * BLOCK_LEN, BLOCK_LEN) for b in range(n_blocks)]
    shape = (BLOCK_LEN, BLOCK_LEN)
    causal = lax.broadcasted_iota(jnp.int32, shape, 0) >= lax.broadcasted_iota(jnp.int32, shape, 1)
    work = []
    for head in range(state_ref.shape[1]):
        cols = pl.ds(head * HEAD_DIM, HEAD_DIM)
        fwd = [state_ref[0, head]]
        for b in range(n_blocks - 1):
            fwd.append(fwd[-1] + dot(k_ref[rows[b], cols], v_ref[rows[b], cols], (0, 0)))
        rev = [state_ref[1, head]]
        for b in range(n_blocks - 1, 0, -1):
            rev.insert(0, rev[0] + dot(q_ref[rows[b], cols], do_ref[rows[b], cols], (0, 0)))
        work += [(rows[b], cols, fwd[b].astype(BF16), rev[b].astype(BF16)) for b in range(n_blocks)]
    scores = []
    for at, cols, s, r in work:
        att = jnp.where(causal, dot(q_ref[at, cols], k_ref[at, cols], (1, 1)), 0.0).astype(BF16)
        d_att = jnp.where(causal, dot(do_ref[at, cols], v_ref[at, cols], (1, 1)), 0.0).astype(BF16)
        scores.append((att, d_att))
    for (at, cols, s, r), (att, d_att) in zip(work, scores):
        q, k, v, do = q_ref[at, cols], k_ref[at, cols], v_ref[at, cols], do_ref[at, cols]
        out_ref[at, cols] = ((dot(att, v, (1, 0)) + dot(q, s, (1, 0))) * scale).astype(BF16)
        late_ref[0, at, cols] = ((dot(d_att, k, (1, 0)) + dot(do, s, (1, 1))) * scale).astype(BF16)
        late_ref[1, at, cols] = ((dot(d_att, q, (0, 0)) + dot(v, r, (1, 1))) * scale).astype(BF16)
        late_ref[2, at, cols] = ((dot(att, do, (0, 0)) + dot(k, r, (1, 0))) * scale).astype(BF16)
    first_half = pl.program_id(0) < pl.num_programs(0) // 2

    @pl.when(first_half)
    def _():
        late_ref[3] = out_ref[...]
        late_ref[4] = dy_ref[...]

    @pl.when(jnp.logical_not(first_half))
    def _():
        late_ref[3] = dy_ref[...]
        late_ref[4] = out_ref[...]


def exchange_kernel(side, halves, early_ref, late_ref, *refs):
    own_outs, other_outs = refs[: 2 * halves], refs[2 * halves : 4 * halves]
    early, near, far, pair_early, pair_late, total, landed, gathered = refs[4 * halves : -9]
    send_sem, recv_sem, early_sem, ring_send, ring_recv, out_sem, swap_send, swap_recv, load_sem = refs[-9:]
    me = lax.axis_index("sp")
    core, sign, at, ahead, behind, wrap = neighbours(me, side)
    partner = me + sign

    barrier = pltpu.get_barrier_semaphore()
    for other in ahead + behind + (partner,):
        pl.semaphore_signal(barrier, inc=1, device_id={"sp": other}, device_id_type=MESH)
    pl.semaphore_wait(barrier, 5)

    half = early_ref.shape[3]
    block = half // N_CORES

    def send(*args):
        copy = remote(*args)
        copy.start()
        return copy

    def late_of(which, part):
        return late_ref.at[which + part * (which // (N_GRADS - 1))]

    copies = {}

    def start(part, kind, src, dst, target):
        copies[part, kind] = send(src, dst, send_sem.at[part, kind], recv_sem.at[part, kind], target)

    for part in range(2):
        start(part, 3, late_of(wrap(at[part] + 2), part), far.at[part], ahead[part])
    for part in range(2):
        start(part, 1, late_of(wrap(at[part] - sign), part), near.at[part, 1], behind[part])
        start(part, 7, late_of(at[part], part), pair_late.at[part, 3], partner)
    for part in range(2):
        start(part, 0, late_of(wrap(at[part] + sign), part), near.at[part, 0], ahead[part])
    load = pltpu.make_async_copy(early_ref, early, load_sem.at[0])
    load.start()
    shares = [send(early_ref.at[part], pair_early.at[part], early_sem.at[0, part], early_sem.at[1, part], partner) for part in range(2)]

    n_tiles = 2
    width = half // n_tiles

    def my_cols(start):
        return pl.ds(pl.multiple_of(start + core * block, block), block)

    def accumulate(part, early_part, late_part, fresh=False):
        def add(left_value, right, offset, right_offset):
            def tile(t, carry):
                cols = pl.ds(pl.multiple_of(offset + t * width, width), width)
                product = dot(left_value, right[:, pl.ds(pl.multiple_of(right_offset + t * width, width), width)], (0, 0))
                if fresh:
                    total[part, :, cols] = product
                else:
                    total[part, :, cols] += product
                return carry

            return tile

        @pl.when(at[part] < N_GRADS - 1)
        def _():
            lax.fori_loop(0, 2 * n_tiles, add(early_part[:, my_cols(0)], late_part, 0, 0), 0)

        @pl.when(at[part] == N_GRADS - 1)
        def _():
            left_value = late_part[:, my_cols(part * half)]
            lax.fori_loop(0, n_tiles, add(left_value, early_part, part * half, 0), 0)
            lax.fori_loop(0, n_tiles, add(left_value, late_part, (1 - part) * half, (1 - part) * half), 0)

    def take(part, slot):
        copies[part, slot].wait_recv()
        start(part, 4 + slot, near.at[part, slot], pair_late.at[part, slot], partner)
        accumulate(part, early.at[part, slot], near.at[part, slot])

    def take_other(part, slot):
        copies[part, 4 + slot].wait_recv()
        accumulate(part, pair_early.at[part, slot], pair_late.at[part, slot])

    load.wait()
    for part in range(2):
        accumulate(part, early.at[part, 3], late_of(at[part], part), fresh=True)
    for part in range(2):
        shares[part].wait_recv()
        take_other(part, 3)
    for part in range(2):
        copies[part, 3].wait_recv()
        start(part, 2, far.at[part], near.at[part, 2], ahead[part])
    for slot in (1, 0, 2):
        for part in range(2):
            take(part, slot)
        for part in range(2):
            take_other(part, slot)

    piece = block // side
    small = piece // halves

    def rows(part, shift, h):
        return pl.ds(pl.multiple_of(wrap(at[1 - part] + sign * shift) * piece + h * small, small), small)

    def ring(part, h, step, src, dst):
        return send(src, dst, ring_send.at[part, h, step], ring_recv.at[part, h, step], ahead[1 - part])

    lanes = [(part, h) for h in range(halves) for part in range(2)]
    hops = {}
    for part, h in lanes:
        hops[part, h, 0] = ring(part, h, 0, total.at[part, rows(part, -1, h)], landed.at[part, h, 0])
    for step in range(1, side - 1):
        for part, h in lanes:
            hops[part, h, step - 1].wait_recv()
            landed[part, h, step - 1] += total[part, rows(part, -(step + 1), h), :]
            hops[part, h, step] = ring(part, h, step, landed.at[part, h, step - 1], landed.at[part, h, step])
    stores = []

    swaps = []

    def store(part, h, shift, n):
        src = gathered.at[part, rows(part, shift, h)]
        where = pl.ds(pl.multiple_of(wrap(at[1 - part] + sign * shift) * small, small), small)
        copy = pltpu.make_async_copy(src, own_outs[2 * h + part].at[where], out_sem.at[part, h, n])
        copy.start()
        stores.append(copy)
        swaps.append(send(src, other_outs[2 * h + part].at[where], swap_send.at[part, h, n], swap_recv.at[part, h, n], partner))

    last = side - 1
    for part, h in lanes:
        hops[part, h, last - 1].wait_recv()
        mine = rows(part, 0, h)
        gathered[part, mine, :] = landed[part, h, last - 1] + total[part, mine, :]
        hops[part, h, last] = ring(part, h, last, gathered.at[part, mine], gathered.at[part, mine])
        store(part, h, 0, 0)
    for step in range(1, side):
        for part, h in lanes:
            hops[part, h, last + step - 1].wait_recv()
            where = rows(part, -step, h)
            if step < side - 1:
                hops[part, h, last + step] = ring(part, h, last + step, gathered.at[part, where], gathered.at[part, where])
            store(part, h, -step, step)
    for copy in stores:
        copy.wait()
    for copy in list(copies.values()) + shares:
        copy.wait_send()
    for copy in hops.values():
        copy.wait_send()
    for copy in swaps:
        copy.wait()


def place_kernel(side, step, lane, halves, kinds, fresh, *refs):
    n_blocks = len(kinds)
    blocks = refs[:n_blocks]
    grads = refs[n_blocks if fresh else n_blocks + N_GRADS :][:N_GRADS]
    buf, sem_in, sem_out = refs[-3:]
    index = lax.axis_index("sp")
    core = lax.rem(index, N_CORES)
    col = lax.rem(index // N_CORES, side)
    row = index // (N_CORES * side)
    small = blocks[0].shape[0] // side
    piece = small * halves
    half = grads[0].shape[0] // 2
    jobs = []
    for (own, part), src in zip(kinds, blocks):
        at = col if part == 0 else row
        c = core if own else 1 - core
        which = lax.rem(at - (1 - 2 * c) * step + 2 * side, side)
        start = part * half + c * side * piece + lane * small
        for g in range(side):
            jobs.append((src.at[pl.ds(g * small, small)], which, pl.multiple_of(start + g * piece, small)))
    for n, (src, which, start) in enumerate(jobs):
        pltpu.make_async_copy(src, buf.at[n], sem_in.at[n]).start()
    for n, (src, which, start) in enumerate(jobs):
        pltpu.make_async_copy(src, buf.at[n], sem_in.at[n]).wait()
        for m in range(N_GRADS):

            @pl.when(which == m)
            def _():
                pltpu.make_async_copy(buf.at[n], grads[m].at[pl.ds(start, small)], sem_out.at[n]).start()

    for n, (src, which, start) in enumerate(jobs):
        pltpu.make_async_copy(buf.at[n], grads[0].at[pl.ds(0, small)], sem_out.at[n]).wait()


def solution(mesh):
    n_seq = mesh.shape["sp"]
    side = math.isqrt(n_seq // N_CORES)
    assert side == N_GRADS
    row_spec = P(("dp", "sp"), None)
    grad_spec = P("dp", None)

    def device_at(row, col, core):
        return ((row % side) * side + col % side) * N_CORES + core

    def ring_perm(axis, hops):
        pairs = []
        for row in range(side):
            for col in range(side):
                for core in range(N_CORES):
                    shift = hops * (1 - 2 * core)
                    target = device_at(row, col + shift, core) if axis == "x" else device_at(row + shift, col, core)
                    pairs.append((device_at(row, col, core), target))
        return pairs

    core_perm = [(j, j ^ 1) for j in range(n_seq)]

    def local_layer(tokens, w_q, w_k, w_v, w_o, grad_y):
        n_rows, model_dim = tokens.shape
        n_heads = model_dim // HEAD_DIM
        att_scale = 1.0 / math.sqrt(n_rows * n_seq * HEAD_DIM)
        index = lax.axis_index("sp")
        core = lax.rem(index, N_CORES)
        place = {"x": lax.rem(index // N_CORES, side), "y": index // (N_CORES * side)}

        def swap_cores(value):
            return lax.ppermute(value, "sp", perm=core_perm)

        def hop(value, axis, hops):
            return lax.ppermute(value, "sp", perm=ring_perm(axis, hops))

        def project(operand, weight):
            return jnp.dot(operand, weight, preferred_element_type=F32).astype(BF16)

        def back_proj(rows, weight):
            return jnp.einsum("ne,de->nd", rows, weight, preferred_element_type=F32)

        tile = 2 * HEAD_DIM
        state_shape = (2, n_heads, HEAD_DIM, HEAD_DIM)
        full = pl.BlockSpec((n_rows, model_dim), lambda i: (0, 0))
        in_cols = pl.BlockSpec((model_dim, tile), lambda i: (0, i))
        in_rows = pl.BlockSpec((tile, model_dim), lambda i: (i, 0))
        out_cols = pl.BlockSpec((n_rows, tile), lambda i: (0, i))
        act = jax.ShapeDtypeStruct((n_rows, model_dim), BF16)
        half = model_dim // 2
        dma = pltpu.SemaphoreType.DMA
        anywhere = pl.BlockSpec(memory_space=pl.ANY)
        n_group = n_heads // N_CORES
        q, k, v, do, early, states = pl.pallas_call(
            functools.partial(project_kernel, side),
            grid=(model_dim // tile,),
            in_specs=[full, full, in_cols, in_cols, in_cols, in_rows, anywhere, anywhere],
            out_specs=[out_cols] * 4 + [anywhere] * 2,
            out_shape=[act] * 4 + [jax.ShapeDtypeStruct((2, 4, n_rows, half), BF16), jax.ShapeDtypeStruct(state_shape, F32)],
            scratch_shapes=[VMEM(state_shape, F32)] * 2
            + [VMEM((2, n_rows, half), BF16), dma((2, 4)), dma((2, 4)), dma((3,))]
            + [VMEM((2, n_group, HEAD_DIM, HEAD_DIM), F32)] * 6
            + [dma((2,))] * 2
            + [dma((2, n_group))] * 4
            + [dma((2, n_group, side - 1))]
            + [dma((2, n_group))] * 2,
            cost_estimate=pl.CostEstimate(flops=8 * n_rows * model_dim * model_dim, bytes_accessed=8 * model_dim * model_dim, transcendentals=0),
            compiler_params=pltpu.CompilerParams(collective_id=3, has_side_effects=True, vmem_limit_bytes=48 * 2**20),
            name="project",
        )(tokens, grad_y, w_q, w_k, w_v, w_o, tokens, grad_y)

        out_rows, late = pl.pallas_call(
            functools.partial(attend_kernel, att_scale),
            grid=(model_dim // tile,),
            in_specs=[out_cols] * 5 + [pl.BlockSpec((2, tile // HEAD_DIM, HEAD_DIM, HEAD_DIM), lambda i: (0, i, 0, 0))],
            out_specs=[out_cols, pl.BlockSpec((5, n_rows, tile), lambda i: (0, 0, i))],
            out_shape=[act, jax.ShapeDtypeStruct((5, n_rows, model_dim), BF16)],
            cost_estimate=pl.CostEstimate(flops=n_heads * 24 * 2 * 128**3, bytes_accessed=2**24, transcendentals=0),
            compiler_params=pltpu.CompilerParams(vmem_limit_bytes=16 * 2**20),
            name="attend",
        )(q, k, v, do, grad_y, states)

        block = half // N_CORES
        halves = 2
        small = block // side // halves
        axes = (("x", "y"), ("y", "x"))
        blocks = pl.pallas_call(
            functools.partial(exchange_kernel, side, halves),
            in_specs=[anywhere, pl.BlockSpec(memory_space=VMEM)],
            out_specs=[anywhere] * (4 * halves),
            out_shape=[jax.ShapeDtypeStruct((block // halves, model_dim), F32)] * (4 * halves),
            scratch_shapes=[
                VMEM((2, 4, n_rows, half), BF16),
                VMEM((2, 3, n_rows, model_dim), BF16),
                VMEM((2, n_rows, model_dim), BF16),
                VMEM((2, 4, n_rows, half), BF16),
                VMEM((2, 4, n_rows, model_dim), BF16),
                VMEM((2, block, model_dim), F32),
                VMEM((2, halves, side - 1, small, model_dim), F32),
                VMEM((2, block, model_dim), F32),
                dma((2, 8)),
                dma((2, 8)),
                dma((2, 2)),
                dma((2, halves, 2 * (side - 1))),
                dma((2, halves, 2 * (side - 1))),
                dma((2, halves, side)),
                dma((2, halves, side)),
                dma((2, halves, side)),
                dma((1,)),
            ],
            cost_estimate=pl.CostEstimate(flops=2 * 2 * block * model_dim * n_rows * 8, bytes_accessed=2**24, transcendentals=0),
            compiler_params=pltpu.CompilerParams(collective_id=1, has_side_effects=True, vmem_limit_bytes=60 * 2**20),
            name="exchange",
        )(early, late)
        own = [list(blocks[2 * h : 2 * h + 2]) for h in range(halves)]
        others = [list(blocks[2 * (halves + h) : 2 * (halves + h) + 2]) for h in range(halves)]

        grads = []

        def put(kinds, sources, step, h):
            n_copies = len(kinds) * side
            return pl.pallas_call(
                functools.partial(place_kernel, side, step, h, halves, kinds, not grads),
                in_specs=[anywhere] * (len(kinds) + len(grads)),
                out_specs=[anywhere] * N_GRADS,
                out_shape=[jax.ShapeDtypeStruct((model_dim, model_dim), F32)] * N_GRADS,
                scratch_shapes=[VMEM((n_copies, small, model_dim), F32), dma((n_copies,)), dma((n_copies,))],
                input_output_aliases={len(kinds) + m: m for m in range(len(grads))},
                cost_estimate=pl.CostEstimate(flops=3 * 10**9, bytes_accessed=8 * n_copies * small * model_dim, transcendentals=0),
            )(*sources, *grads)

        own_kinds, other_kinds = ((True, 0), (True, 1)), ((False, 0), (False, 1))
        for step in range(side):
            for h in range(halves):
                if step:
                    for part, (first, second) in enumerate(axes):
                        own[h][part] = hop(own[h][part], first, 1)
                    for part in range(2):
                        others[h][part] = swap_cores(own[h][part])
                if (step, h) == (side - 1, halves - 1):
                    grads = put(own_kinds, own[h], step, h)
                    grads = put(other_kinds, others[h], step, h)
                else:
                    grads = put(own_kinds + other_kinds, own[h] + others[h], step, h)

        out_y = project(out_rows, w_o)
        grad_x = back_proj(late[0], w_q)
        grad_x = grad_x + back_proj(late[1], w_k)
        grad_x = (grad_x + back_proj(late[2], w_v)).astype(BF16)
        return (out_y, grad_x) + tuple(grads)

    return jax.shard_map(local_layer, mesh=mesh, in_specs=(row_spec, P(), P(), P(), P(), row_spec), out_specs=(row_spec, row_spec, grad_spec, grad_spec, grad_spec, grad_spec), check_vma=False)
```

```python
import functools
import math
import jax
import jax.numpy as jnp
from jax import lax
from jax.experimental import pallas as pl
from jax.experimental.pallas import tpu as pltpu
from jax.sharding import PartitionSpec as P


HEAD_DIM = 128
BLOCK_LEN = 128
N_CORES = 2
N_GRADS = 4
RELAY_STEP = 7
SLOTS = 2


F32 = jnp.float32
BF16 = jnp.bfloat16
VMEM = pltpu.VMEM
MESH = pl.DeviceIdType.MESH


def dot(a, b, dims):
    return lax.dot_general(a, b, ((dims[:1], dims[1:]), ((), ())), preferred_element_type=F32)


def neighbours(me, side):
    core = lax.rem(me, N_CORES)
    sign = 1 - 2 * core
    col = lax.rem(me // N_CORES, side)
    row = me // (N_CORES * side)

    def wrap(value):
        return lax.rem(value + 2 * side, side)

    def device(r, c):
        return (r * side + c) * N_CORES + core

    ahead = (device(row, wrap(col + sign)), device(wrap(row + sign), col))
    behind = (device(row, wrap(col - sign)), device(wrap(row - sign), col))
    return core, sign, (col, row), ahead, behind, wrap


def remote(src, dst, send, recv, target):
    return pltpu.make_async_remote_copy(src_ref=src, dst_ref=dst, send_sem=send, recv_sem=recv, device_id={"sp": target}, device_id_type=MESH)


def chain(side, totals_ref, out_ref, other, before, stage, above, down, peer, swap_send, swap_recv, row_send, row_recv, above_recv, down_send, cast_send, back_send, back_recv):
    me = lax.axis_index("sp")
    core = lax.rem(me, N_CORES)
    col = lax.rem(me // N_CORES, side)
    row = me // (N_CORES * side)
    partner = me + 1 - 2 * core
    n_group = totals_ref.shape[1] // N_CORES
    mine, yours = core * n_group, (1 - core) * n_group

    def wrap(value):
        return lax.rem(value + 2 * side, side)

    def device(r, c):
        return (wrap(r) * side + wrap(c)) * N_CORES + core

    def copy(src, dst, send, recv, target):
        return pltpu.make_async_remote_copy(src_ref=src, dst_ref=dst, send_sem=send, recv_sem=recv, device_id={"sp": target}, device_id_type=MESH)

    def swap_copy(kind):
        return copy(totals_ref.at[kind, pl.ds(yours, n_group)], other.at[kind], swap_send.at[kind], swap_recv.at[kind], partner)

    def row_copy(kind, h):
        return copy(stage.at[kind, h], before.at[kind, h], row_send.at[kind, h], row_recv.at[kind, h], device(row, col + 1 - 2 * kind))

    def down_copy(kind, h):
        return copy(down.at[kind, h], above.at[kind, h], down_send.at[kind, h], above_recv.at[kind, h], device(row + 1 - 2 * kind, col))

    def cast_copy(kind, h, n):
        along = (1 - 2 * kind) * (1, -1, 1 - 2 * core)[n]
        return copy(above.at[kind, h], above.at[kind, h], cast_send.at[kind, h, n], above_recv.at[kind, h], device(row, col + along))

    def back_copy(kind, h):
        return copy(peer.at[kind, h], out_ref.at[kind, mine + h], back_send.at[kind, h], back_recv.at[kind, h], partner)

    def position(kind, coordinate):
        return kind * (side - 1) + (1 - 2 * kind) * coordinate

    for kind in range(2):
        swap_copy(kind).start()
    for kind in range(2):

        @pl.when(position(kind, col) == 0)
        def _():
            before[kind] = jnp.zeros_like(before[kind])

        @pl.when((position(kind, col) == side - 1) & (position(kind, row) == 0))
        def _():
            above[kind] = jnp.zeros_like(above[kind])

    for kind in range(2):
        swap_copy(kind).wait()

    def run(slot, carry):
        for kind in range(2):
            along, across = position(kind, col), position(kind, row)
            h = slot - SLOTS * along

            @pl.when((h >= 0) & (h < n_group))
            def _():
                @pl.when(along > 0)
                def _():
                    row_copy(kind, h).wait_recv()

                stage[kind, h] = before[kind, h] + (totals_ref[kind, mine + h] + other[kind, h])

                @pl.when(along < side - 1)
                def _():
                    row_copy(kind, h).start()

            g = slot - SLOTS * (side - 1 + across)

            @pl.when((along == side - 1) & (g >= 0) & (g < n_group))
            def _():
                @pl.when(across > 0)
                def _():
                    down_copy(kind, g).wait_recv()

                @pl.when(across < side - 1)
                def _():
                    down[kind, g] = above[kind, g] + stage[kind, g]
                    down_copy(kind, g).start()

                for n in range(2):
                    cast_copy(kind, g, n).start()

        return carry

    lax.fori_loop(0, 2 * SLOTS * (side - 1) + n_group, run, 0)

    def finish(h, carry):
        for i in range(2):
            kind = lax.rem(1 - col // (side // 2) + i, 2)
            along = position(kind, col)

            @pl.when(along < side - 1)
            def _():
                down_copy(kind, h).wait_recv()

            @pl.when(along == 2 * core)
            def _():
                cast_copy(kind, h, 2).start()

        for kind in range(2):
            base = above[kind, h] + before[kind, h]
            own_total, other_total = totals_ref[kind, mine + h], other[kind, h]
            out_ref[kind, mine + h] = jnp.where(core == kind, base, base + other_total)
            peer[kind, h] = jnp.where(core == kind, base + own_total, base)
            back_copy(kind, h).start()
        return carry

    lax.fori_loop(0, n_group, finish, 0)

    def drain(h, carry):
        for kind in range(2):
            along, across = position(kind, col), position(kind, row)
            back_copy(kind, h).wait()

            @pl.when(along == 2 * core)
            def _():
                cast_copy(kind, h, 2).wait_send()

            @pl.when(along < side - 1)
            def _():
                row_copy(kind, h).wait_send()

            @pl.when(along == side - 1)
            def _():
                for n in range(2):
                    cast_copy(kind, h, n).wait_send()

                @pl.when(across < side - 1)
                def _():
                    down_copy(kind, h).wait_send()

        return carry

    lax.fori_loop(0, n_group, drain, 0)


def project_kernel(side, x_ref, dy_ref, wq_ref, wk_ref, wv_ref, wo_ref, x_any, dy_any, q_ref, k_ref, v_ref, do_ref, early_ref, states_ref, totals, states, relay, send_sem, recv_sem, own_sem, *chain_refs):
    core, sign, at, ahead, behind, wrap = neighbours(lax.axis_index("sp"), side)
    half = early_ref.shape[3]
    step = pl.program_id(0)

    def early(part, kind, src):
        dst = relay.at[part] if kind == 3 else early_ref.at[part, kind]
        return remote(src, dst, send_sem.at[part, kind], recv_sem.at[part, kind], behind[part] if kind == 1 else ahead[part])

    def source(part, array):
        return array.at[:, pl.ds(part * half, half)]

    def start_to(part, kind, which):
        @pl.when(which < N_GRADS - 1)
        def _():
            early(part, kind, source(part, x_any)).start()

        @pl.when(which == N_GRADS - 1)
        def _():
            early(part, kind, source(part, dy_any)).start()

    def own(part, array):
        return pltpu.make_async_copy(source(part, array), early_ref.at[part, 3], own_sem.at[part])

    @pl.when(step == 0)
    def _():
        barrier = pltpu.get_barrier_semaphore()
        me = lax.axis_index("sp")
        first_in_row = at[1] * side * N_CORES + core
        peers = [first_in_row + wrap(at[0] + t) * N_CORES for t in range(1, side)] + [ahead[1], behind[1], me + sign]
        for target in peers:
            pl.semaphore_signal(barrier, inc=1, device_id={"sp": target}, device_id_type=MESH)
        pl.semaphore_wait(barrier, len(peers))
        for part in range(2):
            start_to(part, 3, wrap(at[part] + 2))
        for part in range(2):
            start_to(part, 1, wrap(at[part] - sign))
        for part in range(2):
            start_to(part, 0, wrap(at[part] + sign))

            @pl.when(at[part] < N_GRADS - 1)
            def _():
                own(part, x_any).start()

            @pl.when(at[part] == N_GRADS - 1)
            def _():
                own(part, dy_any).start()

    @pl.when(step == RELAY_STEP)
    def _():
        for part in range(2):
            early(part, 3, source(part, x_any)).wait_recv()
            early(part, 2, relay.at[part]).start()

    x = x_ref[...]
    q_ref[...] = dot(x, wq_ref[...], (1, 0)).astype(BF16)
    k_ref[...] = dot(x, wk_ref[...], (1, 0)).astype(BF16)
    v_ref[...] = dot(x, wv_ref[...], (1, 0)).astype(BF16)
    do_ref[...] = dot(dy_ref[...], wo_ref[...], (1, 1)).astype(BF16)
    for head in range(q_ref.shape[1] // HEAD_DIM):
        cols = slice(head * HEAD_DIM, (head + 1) * HEAD_DIM)
        kv = dot(k_ref[:, cols], v_ref[:, cols], (0, 0))
        qdo = dot(q_ref[:, cols], do_ref[:, cols], (0, 0))
        at_head = step * (q_ref.shape[1] // HEAD_DIM) + head
        totals[0, at_head] = kv
        totals[1, at_head] = qdo

    @pl.when(step == pl.num_programs(0) - 1)
    def _():
        chain(side, totals, states, *chain_refs)
        result = pltpu.make_async_copy(states, states_ref, own_sem.at[2])
        result.start()
        result.wait()
        for part in range(2):
            own(part, x_any).wait()
            for kind in range(4):
                copy = early(part, kind, source(part, x_any))
                copy.wait_send()
                if kind != 3:
                    copy.wait_recv()


def attend_kernel(scale, q_ref, k_ref, v_ref, do_ref, dy_ref, state_ref, out_ref, late_ref):
    n_blocks = q_ref.shape[0] // BLOCK_LEN
    rows = [pl.ds(b * BLOCK_LEN, BLOCK_LEN) for b in range(n_blocks)]
    shape = (BLOCK_LEN, BLOCK_LEN)
    causal = lax.broadcasted_iota(jnp.int32, shape, 0) >= lax.broadcasted_iota(jnp.int32, shape, 1)
    work = []
    for head in range(state_ref.shape[1]):
        cols = pl.ds(head * HEAD_DIM, HEAD_DIM)
        fwd = [state_ref[0, head]]
        for b in range(n_blocks - 1):
            fwd.append(fwd[-1] + dot(k_ref[rows[b], cols], v_ref[rows[b], cols], (0, 0)))
        rev = [state_ref[1, head]]
        for b in range(n_blocks - 1, 0, -1):
            rev.insert(0, rev[0] + dot(q_ref[rows[b], cols], do_ref[rows[b], cols], (0, 0)))
        work += [(rows[b], cols, fwd[b].astype(BF16), rev[b].astype(BF16)) for b in range(n_blocks)]
    scores = []
    for at, cols, s, r in work:
        att = jnp.where(causal, dot(q_ref[at, cols], k_ref[at, cols], (1, 1)), 0.0).astype(BF16)
        d_att = jnp.where(causal, dot(do_ref[at, cols], v_ref[at, cols], (1, 1)), 0.0).astype(BF16)
        scores.append((att, d_att))
    for (at, cols, s, r), (att, d_att) in zip(work, scores):
        q, k, v, do = q_ref[at, cols], k_ref[at, cols], v_ref[at, cols], do_ref[at, cols]
        out_ref[at, cols] = ((dot(att, v, (1, 0)) + dot(q, s, (1, 0))) * scale).astype(BF16)
        late_ref[0, at, cols] = ((dot(d_att, k, (1, 0)) + dot(do, s, (1, 1))) * scale).astype(BF16)
        late_ref[1, at, cols] = ((dot(d_att, q, (0, 0)) + dot(v, r, (1, 1))) * scale).astype(BF16)
        late_ref[2, at, cols] = ((dot(att, do, (0, 0)) + dot(k, r, (1, 0))) * scale).astype(BF16)
    first_half = pl.program_id(0) < pl.num_programs(0) // 2

    @pl.when(first_half)
    def _():
        late_ref[3] = out_ref[...]
        late_ref[4] = dy_ref[...]

    @pl.when(jnp.logical_not(first_half))
    def _():
        late_ref[3] = dy_ref[...]
        late_ref[4] = out_ref[...]


def exchange_kernel(side, halves, early_ref, late_ref, *refs):
    own_outs, other_outs = refs[: 2 * halves], refs[2 * halves : 4 * halves]
    early, own_late, near, far, pair_early, pair_late, total, landed, gathered = refs[4 * halves : -9]
    send_sem, recv_sem, early_sem, ring_send, ring_recv, out_sem, swap_send, swap_recv, load_sem = refs[-9:]
    me = lax.axis_index("sp")
    core, sign, at, ahead, behind, wrap = neighbours(me, side)
    partner = me + sign

    barrier = pltpu.get_barrier_semaphore()
    for other in ahead + behind + (partner,):
        pl.semaphore_signal(barrier, inc=1, device_id={"sp": other}, device_id_type=MESH)
    pl.semaphore_wait(barrier, 5)

    half = early_ref.shape[3]
    block = half // N_CORES

    def send(*args):
        copy = remote(*args)
        copy.start()
        return copy

    def late_of(which, part):
        return late_ref.at[which + part * (which // (N_GRADS - 1))]

    copies = {}

    def start(part, kind, src, dst, target):
        copies[part, kind] = send(src, dst, send_sem.at[part, kind], recv_sem.at[part, kind], target)

    for part in range(2):
        start(part, 3, late_of(wrap(at[part] + 2), part), far.at[part], ahead[part])
    for part in range(2):
        start(part, 1, late_of(wrap(at[part] - sign), part), near.at[part, 1], behind[part])
        start(part, 7, late_of(at[part], part), pair_late.at[part, 3], partner)
    for part in range(2):
        start(part, 0, late_of(wrap(at[part] + sign), part), near.at[part, 0], ahead[part])
    load = pltpu.make_async_copy(early_ref, early, load_sem.at[0])
    load.start()
    own_loads = [pltpu.make_async_copy(late_of(at[part], part), own_late.at[part], load_sem.at[1 + part]) for part in range(2)]
    for own_load in own_loads:
        own_load.start()
    shares = [send(early_ref.at[part], pair_early.at[part], early_sem.at[0, part], early_sem.at[1, part], partner) for part in range(2)]

    n_tiles = 2
    width = half // n_tiles

    def my_cols(start):
        return pl.ds(pl.multiple_of(start + core * block, block), block)

    def accumulate(part, early_part, late_part, fresh=False):
        def add(left_value, right, offset, right_offset):
            def tile(t, carry):
                cols = pl.ds(pl.multiple_of(offset + t * width, width), width)
                product = dot(left_value, right[:, pl.ds(pl.multiple_of(right_offset + t * width, width), width)], (0, 0))
                if fresh:
                    total[part, :, cols] = product
                else:
                    total[part, :, cols] += product
                return carry

            return tile

        @pl.when(at[part] < N_GRADS - 1)
        def _():
            lax.fori_loop(0, 2 * n_tiles, add(early_part[:, my_cols(0)], late_part, 0, 0), 0)

        @pl.when(at[part] == N_GRADS - 1)
        def _():
            left_value = late_part[:, my_cols(part * half)]
            lax.fori_loop(0, n_tiles, add(left_value, early_part, part * half, 0), 0)
            lax.fori_loop(0, n_tiles, add(left_value, late_part, (1 - part) * half, (1 - part) * half), 0)

    def take(part, slot):
        copies[part, slot].wait_recv()
        start(part, 4 + slot, near.at[part, slot], pair_late.at[part, slot], partner)
        accumulate(part, early.at[part, slot], near.at[part, slot])

    def take_other(part, slot):
        copies[part, 4 + slot].wait_recv()
        accumulate(part, pair_early.at[part, slot], pair_late.at[part, slot])

    load.wait()
    for part in range(2):
        own_loads[part].wait()
        accumulate(part, early.at[part, 3], own_late.at[part], fresh=True)
    for part in range(2):
        shares[part].wait_recv()
        take_other(part, 3)
    for part in range(2):
        copies[part, 3].wait_recv()
        start(part, 2, far.at[part], near.at[part, 2], ahead[part])
    for slot in (1, 0, 2):
        for part in range(2):
            take(part, slot)
        for part in range(2):
            take_other(part, slot)

    piece = block // side
    small = piece // halves

    def rows(part, shift, h):
        return pl.ds(pl.multiple_of(wrap(at[1 - part] + sign * shift) * piece + h * small, small), small)

    def ring(part, h, step, src, dst):
        return send(src, dst, ring_send.at[part, h, step], ring_recv.at[part, h, step], ahead[1 - part])

    lanes = [(part, h) for h in range(halves) for part in range(2)]
    hops = {}
    for part, h in lanes:
        hops[part, h, 0] = ring(part, h, 0, total.at[part, rows(part, -1, h)], landed.at[part, h, 0])
    for step in range(1, side - 1):
        for part, h in lanes:
            hops[part, h, step - 1].wait_recv()
            landed[part, h, step - 1] += total[part, rows(part, -(step + 1), h), :]
            hops[part, h, step] = ring(part, h, step, landed.at[part, h, step - 1], landed.at[part, h, step])
    stores = []

    swaps = []

    def store(part, h, shift, n):
        src = gathered.at[part, rows(part, shift, h)]
        where = pl.ds(pl.multiple_of(wrap(at[1 - part] + sign * shift) * small, small), small)
        copy = pltpu.make_async_copy(src, own_outs[2 * h + part].at[where], out_sem.at[part, h, n])
        copy.start()
        stores.append(copy)
        swaps.append(send(src, other_outs[2 * h + part].at[where], swap_send.at[part, h, n], swap_recv.at[part, h, n], partner))

    last = side - 1
    for part, h in lanes:
        hops[part, h, last - 1].wait_recv()
        mine = rows(part, 0, h)
        gathered[part, mine, :] = landed[part, h, last - 1] + total[part, mine, :]
        hops[part, h, last] = ring(part, h, last, gathered.at[part, mine], gathered.at[part, mine])
        store(part, h, 0, 0)
    for step in range(1, side):
        for part, h in lanes:
            hops[part, h, last + step - 1].wait_recv()
            where = rows(part, -step, h)
            if step < side - 1:
                hops[part, h, last + step] = ring(part, h, last + step, gathered.at[part, where], gathered.at[part, where])
            store(part, h, -step, step)
    for copy in stores:
        copy.wait()
    for copy in list(copies.values()) + shares:
        copy.wait_send()
    for copy in hops.values():
        copy.wait_send()
    for copy in swaps:
        copy.wait()


def place_kernel(side, step, lane, halves, kinds, fresh, *refs):
    n_blocks = len(kinds)
    blocks = refs[:n_blocks]
    grads = refs[n_blocks if fresh else n_blocks + N_GRADS :][:N_GRADS]
    buf, sem_in, sem_out = refs[-3:]
    index = lax.axis_index("sp")
    core = lax.rem(index, N_CORES)
    col = lax.rem(index // N_CORES, side)
    row = index // (N_CORES * side)
    small = blocks[0].shape[0] // side
    piece = small * halves
    half = grads[0].shape[0] // 2
    jobs = []
    for (own, part), src in zip(kinds, blocks):
        at = col if part == 0 else row
        c = core if own else 1 - core
        which = lax.rem(at - (1 - 2 * c) * step + 2 * side, side)
        start = part * half + c * side * piece + lane * small
        for g in range(side):
            jobs.append((src.at[pl.ds(g * small, small)], which, pl.multiple_of(start + g * piece, small)))
    for n, (src, which, start) in enumerate(jobs):
        pltpu.make_async_copy(src, buf.at[n], sem_in.at[n]).start()
    for n, (src, which, start) in enumerate(jobs):
        pltpu.make_async_copy(src, buf.at[n], sem_in.at[n]).wait()
        for m in range(N_GRADS):

            @pl.when(which == m)
            def _():
                pltpu.make_async_copy(buf.at[n], grads[m].at[pl.ds(start, small)], sem_out.at[n]).start()

    for n, (src, which, start) in enumerate(jobs):
        pltpu.make_async_copy(buf.at[n], grads[0].at[pl.ds(0, small)], sem_out.at[n]).wait()


def solution(mesh):
    n_seq = mesh.shape["sp"]
    side = math.isqrt(n_seq // N_CORES)
    assert side == N_GRADS
    row_spec = P(("dp", "sp"), None)
    grad_spec = P("dp", None)

    def device_at(row, col, core):
        return ((row % side) * side + col % side) * N_CORES + core

    def ring_perm(axis, hops):
        pairs = []
        for row in range(side):
            for col in range(side):
                for core in range(N_CORES):
                    shift = hops * (1 - 2 * core)
                    target = device_at(row, col + shift, core) if axis == "x" else device_at(row + shift, col, core)
                    pairs.append((device_at(row, col, core), target))
        return pairs

    core_perm = [(j, j ^ 1) for j in range(n_seq)]

    def local_layer(tokens, w_q, w_k, w_v, w_o, grad_y):
        n_rows, model_dim = tokens.shape
        n_heads = model_dim // HEAD_DIM
        att_scale = 1.0 / math.sqrt(n_rows * n_seq * HEAD_DIM)
        index = lax.axis_index("sp")
        core = lax.rem(index, N_CORES)
        place = {"x": lax.rem(index // N_CORES, side), "y": index // (N_CORES * side)}

        def swap_cores(value):
            return lax.ppermute(value, "sp", perm=core_perm)

        def hop(value, axis, hops):
            return lax.ppermute(value, "sp", perm=ring_perm(axis, hops))

        def project(operand, weight):
            return jnp.dot(operand, weight, preferred_element_type=F32).astype(BF16)

        def back_proj(rows, weight):
            return jnp.einsum("ne,de->nd", rows, weight, preferred_element_type=F32)

        tile = 2 * HEAD_DIM
        state_shape = (2, n_heads, HEAD_DIM, HEAD_DIM)
        full = pl.BlockSpec((n_rows, model_dim), lambda i: (0, 0))
        in_cols = pl.BlockSpec((model_dim, tile), lambda i: (0, i))
        in_rows = pl.BlockSpec((tile, model_dim), lambda i: (i, 0))
        out_cols = pl.BlockSpec((n_rows, tile), lambda i: (0, i))
        act = jax.ShapeDtypeStruct((n_rows, model_dim), BF16)
        half = model_dim // 2
        dma = pltpu.SemaphoreType.DMA
        anywhere = pl.BlockSpec(memory_space=pl.ANY)
        n_group = n_heads // N_CORES
        q, k, v, do, early, states = pl.pallas_call(
            functools.partial(project_kernel, side),
            grid=(model_dim // tile,),
            in_specs=[full, full, in_cols, in_cols, in_cols, in_rows, anywhere, anywhere],
            out_specs=[out_cols] * 4 + [anywhere] * 2,
            out_shape=[act] * 4 + [jax.ShapeDtypeStruct((2, 4, n_rows, half), BF16), jax.ShapeDtypeStruct(state_shape, F32)],
            scratch_shapes=[VMEM(state_shape, F32)] * 2
            + [VMEM((2, n_rows, half), BF16), dma((2, 4)), dma((2, 4)), dma((3,))]
            + [VMEM((2, n_group, HEAD_DIM, HEAD_DIM), F32)] * 6
            + [dma((2,))] * 2
            + [dma((2, n_group))] * 4
            + [dma((2, n_group, side - 1))]
            + [dma((2, n_group))] * 2,
            cost_estimate=pl.CostEstimate(flops=8 * n_rows * model_dim * model_dim, bytes_accessed=8 * model_dim * model_dim, transcendentals=0),
            compiler_params=pltpu.CompilerParams(collective_id=3, has_side_effects=True, vmem_limit_bytes=48 * 2**20),
            name="project",
        )(tokens, grad_y, w_q, w_k, w_v, w_o, tokens, grad_y)

        out_rows, late = pl.pallas_call(
            functools.partial(attend_kernel, att_scale),
            grid=(model_dim // tile,),
            in_specs=[out_cols] * 5 + [pl.BlockSpec((2, tile // HEAD_DIM, HEAD_DIM, HEAD_DIM), lambda i: (0, i, 0, 0))],
            out_specs=[out_cols, pl.BlockSpec((5, n_rows, tile), lambda i: (0, 0, i))],
            out_shape=[act, jax.ShapeDtypeStruct((5, n_rows, model_dim), BF16)],
            cost_estimate=pl.CostEstimate(flops=n_heads * 24 * 2 * 128**3, bytes_accessed=2**24, transcendentals=0),
            compiler_params=pltpu.CompilerParams(vmem_limit_bytes=16 * 2**20),
            name="attend",
        )(q, k, v, do, grad_y, states)

        block = half // N_CORES
        halves = 2
        small = block // side // halves
        axes = (("x", "y"), ("y", "x"))
        blocks = pl.pallas_call(
            functools.partial(exchange_kernel, side, halves),
            in_specs=[anywhere, anywhere],
            out_specs=[anywhere] * (4 * halves),
            out_shape=[jax.ShapeDtypeStruct((block // halves, model_dim), F32)] * (4 * halves),
            scratch_shapes=[
                VMEM((2, 4, n_rows, half), BF16),
                VMEM((2, n_rows, model_dim), BF16),
                VMEM((2, 3, n_rows, model_dim), BF16),
                VMEM((2, n_rows, model_dim), BF16),
                VMEM((2, 4, n_rows, half), BF16),
                VMEM((2, 4, n_rows, model_dim), BF16),
                VMEM((2, block, model_dim), F32),
                VMEM((2, halves, side - 1, small, model_dim), F32),
                VMEM((2, block, model_dim), F32),
                dma((2, 8)),
                dma((2, 8)),
                dma((2, 2)),
                dma((2, halves, 2 * (side - 1))),
                dma((2, halves, 2 * (side - 1))),
                dma((2, halves, side)),
                dma((2, halves, side)),
                dma((2, halves, side)),
                dma((3,)),
            ],
            cost_estimate=pl.CostEstimate(flops=2 * 2 * block * model_dim * n_rows * 8, bytes_accessed=2**24, transcendentals=0),
            compiler_params=pltpu.CompilerParams(collective_id=1, has_side_effects=True, vmem_limit_bytes=60 * 2**20),
            name="exchange",
        )(early, late)
        own = [list(blocks[2 * h : 2 * h + 2]) for h in range(halves)]
        others = [list(blocks[2 * (halves + h) : 2 * (halves + h) + 2]) for h in range(halves)]

        grads = []

        def put(kinds, sources, step, h):
            n_copies = len(kinds) * side
            return pl.pallas_call(
                functools.partial(place_kernel, side, step, h, halves, kinds, not grads),
                in_specs=[anywhere] * (len(kinds) + len(grads)),
                out_specs=[anywhere] * N_GRADS,
                out_shape=[jax.ShapeDtypeStruct((model_dim, model_dim), F32)] * N_GRADS,
                scratch_shapes=[VMEM((n_copies, small, model_dim), F32), dma((n_copies,)), dma((n_copies,))],
                input_output_aliases={len(kinds) + m: m for m in range(len(grads))},
                cost_estimate=pl.CostEstimate(flops=3 * 10**9, bytes_accessed=8 * n_copies * small * model_dim, transcendentals=0),
            )(*sources, *grads)

        own_kinds, other_kinds = ((True, 0), (True, 1)), ((False, 0), (False, 1))
        for step in range(side):
            for h in range(halves):
                if step:
                    for part, (first, second) in enumerate(axes):
                        own[h][part] = hop(own[h][part], first, 1)
                    for part in range(2):
                        others[h][part] = swap_cores(own[h][part])
                if (step, h) == (side - 1, halves - 1):
                    grads = put(own_kinds, own[h], step, h)
                    grads = put(other_kinds, others[h], step, h)
                else:
                    grads = put(own_kinds + other_kinds, own[h] + others[h], step, h)

        out_y = project(out_rows, w_o)
        grad_x = back_proj(late[0], w_q)
        grad_x = grad_x + back_proj(late[1], w_k)
        grad_x = (grad_x + back_proj(late[2], w_v)).astype(BF16)
        return (out_y, grad_x) + tuple(grads)

    return jax.shard_map(local_layer, mesh=mesh, in_specs=(row_spec, P(), P(), P(), P(), row_spec), out_specs=(row_spec, row_spec, grad_spec, grad_spec, grad_spec, grad_spec), check_vma=False)
```
